256 devices in a mesh: rep: 32 (over z, y), nodes: 8 (over x, core).
Axes of the slice: x: 4, y: 4, z: 8, core: 2. Of those that a mesh axis runs over, the one named last changes fastest.
Arguments:
- adjacency: bfloat16 [16384, 16384], P('nodes')
- features: bfloat16 [16384, 128], P(('nodes', 'rep'))
- w_one: float32 [128, 256], replicated
- w_two: float32 [256, 172], replicated
- labels: int32 [16384], P(('nodes', 'rep'))
- label_mask: int32 [16384], P(('nodes', 'rep'))
Outputs:
- output 1: float32 [], replicated
- output 2: float32 [128, 256], replicated
- output 3: float32 [256, 172], replicated
All inputs are finite; a program needn't handle non-finite values.
Results may differ from the reference program's by a relative error of at most 0.001.
Values are sent between devices in bfloat16 or wider.
A program may use at most 768 MiB of HBM per device.

```python
import jax
import jax.numpy as jnp
from jax import lax

NUM_NODES = 16384
F_IN = 128
HIDDEN = 256
CLASSES = 172
ROW_BLOCK = 2048
NUM_BLOCKS = NUM_NODES // ROW_BLOCK


def draw_graph(graph_key):
    comm_key, act_key, edge_key = jax.random.split(graph_key, 3)
    community = jax.random.randint(comm_key, (NUM_NODES,), 0, 8)
    activity = jax.random.randint(act_key, (NUM_NODES,), 1, 5)
    node_ids = jnp.arange(NUM_NODES)

    def adj_block(block_index):
        row_start = block_index * ROW_BLOCK
        row_comm = lax.dynamic_slice(community, (row_start,), (ROW_BLOCK,))
        row_act = lax.dynamic_slice(activity, (row_start,), (ROW_BLOCK,))
        edge_draw = jax.random.randint(jax.random.fold_in(edge_key, block_index), (ROW_BLOCK, NUM_NODES), 0, 1000)
        threshold = jnp.where(row_comm[:, None] == community[None, :], 400, 60) * row_act[:, None] // 4
        self_loop = (row_start + jnp.arange(ROW_BLOCK))[:, None] == node_ids[None, :]
        edge_weight = jnp.logical_or(edge_draw < threshold, self_loop).astype(jnp.float32)
        return (edge_weight / jnp.sum(edge_weight, axis=1, keepdims=True)).astype(jnp.bfloat16)

    adjacency = lax.map(adj_block, jnp.arange(NUM_BLOCKS)).reshape(NUM_NODES, NUM_NODES)
    return adjacency, community


def draw_labels(label_key, mask_key):
    labels = jax.random.randint(label_key, (NUM_NODES,), 0, CLASSES)
    mask_draw = (jax.random.randint(mask_key, (NUM_NODES,), 0, 10) < 3).astype(jnp.int32)
    label_mask = jnp.where(jnp.arange(NUM_NODES) == 0, 1, mask_draw).astype(jnp.int32)
    return labels, label_mask


def setup_inputs(seed: int = 0) -> dict:
    root_key = jax.random.key(seed)
    graph_key, mean_key, noise_key, one_key, two_key, label_key, mask_key = jax.random.split(root_key, 7)
    adjacency, community = draw_graph(graph_key)
    comm_mean = jax.random.normal(mean_key, (8, F_IN), jnp.float32)
    feat_noise = jax.random.normal(noise_key, (NUM_NODES, F_IN), jnp.float32)
    features = (comm_mean[community] + feat_noise).astype(jnp.bfloat16)
    w_one = jax.random.normal(one_key, (F_IN, HIDDEN), jnp.float32) * F_IN ** -0.5
    w_two = jax.random.normal(two_key, (HIDDEN, CLASSES), jnp.float32) * HIDDEN ** -0.5
    labels, label_mask = draw_labels(label_key, mask_key)
    return {"adjacency": adjacency, "features": features, "w_one": w_one, "w_two": w_two, "labels": labels, "label_mask": label_mask}


def reference(adjacency, features, w_one, w_two, labels, label_mask):
    adj_blocks = adjacency.reshape(NUM_BLOCKS, ROW_BLOCK, NUM_NODES)

    def aggregate(values):
        def one_block(adj_blk):
            return jnp.dot(adj_blk, values, preferred_element_type=jnp.float32)
        return lax.map(one_block, adj_blocks).reshape(NUM_NODES, values.shape[1])

    def aggregate_t(grad_rows):
        grad_blocks = grad_rows.reshape(NUM_BLOCKS, ROW_BLOCK, grad_rows.shape[1])

        def body(acc, pair):
            adj_blk, grad_blk = pair
            contrib = lax.dot_general(adj_blk, grad_blk, (((0,), (0,)), ((), ())), preferred_element_type=jnp.float32)
            return acc + contrib, None

        init = jnp.zeros((NUM_NODES, grad_rows.shape[1]), jnp.float32)
        return lax.scan(body, init, (adj_blocks, grad_blocks))[0]

    w_one_b = w_one.astype(jnp.bfloat16)
    w_two_b = w_two.astype(jnp.bfloat16)
    y_one = jnp.dot(features, w_one_b, preferred_element_type=jnp.float32).astype(jnp.bfloat16)
    z_one = aggregate(y_one)
    h_one = jnp.maximum(z_one, 0.0).astype(jnp.bfloat16)
    y_two = jnp.dot(h_one, w_two_b, preferred_element_type=jnp.float32).astype(jnp.bfloat16)
    z_two = aggregate(y_two)
    log_probs = jax.nn.log_softmax(z_two, axis=-1)
    onehot = (labels[:, None] == jnp.arange(CLASSES)[None, :]).astype(jnp.float32)
    mask_f = label_mask.astype(jnp.float32)
    label_count = jnp.sum(mask_f)
    loss_value = -jnp.sum(mask_f * jnp.sum(onehot * log_probs, axis=-1)) / label_count
    g_two = ((jnp.exp(log_probs) - onehot) * (mask_f / label_count)[:, None]).astype(jnp.bfloat16)
    dy_two = aggregate_t(g_two).astype(jnp.bfloat16)
    dw_two = lax.dot_general(h_one, dy_two, (((0,), (0,)), ((), ())), preferred_element_type=jnp.float32)
    dh_one = jnp.dot(dy_two, w_two_b.T, preferred_element_type=jnp.float32)
    g_one = jnp.where(z_one > 0, dh_one, 0.0).astype(jnp.bfloat16)
    dy_one = aggregate_t(g_one).astype(jnp.bfloat16)
    dw_one = lax.dot_general(features, dy_one, (((0,), (0,)), ((), ())), preferred_element_type=jnp.float32)
    return (loss_value, dw_one, dw_two)
```

```python
import functools

import jax
import jax.numpy as jnp
from jax import lax
from jax.experimental import pallas as pl
from jax.experimental.pallas import tpu as pltpu
from jax.sharding import PartitionSpec as P

BF = jnp.bfloat16
F32 = jnp.float32
BLK = 64
NEG = -1e30


def ring_order(n):
    return sorted(range(1, n), key=lambda d: (min(d, n - d), d))


def step_kernel(ZN, YN, XN, a_hbm, x_ref, w1_ref, w2_ref, lab_ref, msk_ref, loss_ref, dw1_ref, dw2_ref,
                af, ac, ab, at, xg, yg, y2g, g2g, g1g, zp, zr, dp, dr, ds_, dx, pay, payd, payx, payy, payz,
                mt, mz, mx, my, mc, z1s, h1s, y2pad, w2p,
                sem_af, sem_ab, zs, zrv, as_, arv, cs, crv, rs, rrv, ms, mrv, fs, frv):
    rep_n, node_n = ZN * YN, 2 * XN
    r, i = lax.axis_index("rep"), lax.axis_index("nodes")
    z, y = r // YN, lax.rem(r, YN)
    x, c = i // 2, lax.rem(i, 2)
    classes = w2_ref.shape[1]
    hidden = w1_ref.shape[1]
    zero = jnp.int32(0)

    def dev(dz=0, dy=0, dx_=0, dc=0):
        zz = lax.rem(z + dz, ZN)
        yy = lax.rem(y + dy, YN)
        xx = lax.rem(x + dx_, XN)
        cc = lax.rem(c + dc, 2)
        return {"rep": zz * YN + yy, "nodes": xx * 2 + cc}

    z_order, y_order, x_order = ring_order(ZN), ring_order(YN), ring_order(XN)
    peers = [dev(dz=d) for d in z_order] + [dev(dy=d) for d in y_order] + [dev(dx_=d) for d in x_order] + [dev(dc=1)]

    rows_z = YN * BLK
    n_q = node_n * ZN

    @pl.loop(0, n_q)
    def _(q):
        pltpu.make_async_copy(
            a_hbm.at[pl.ds(pl.multiple_of(z * rows_z, rows_z), rows_z),
                     pl.ds(pl.multiple_of(q * (YN * BLK) + (y // 2) * 128, 128), 128)],
            af.at[:, pl.ds(pl.multiple_of(q * 128, 128), 128)], sem_af).start()

    @pl.loop(0, node_n)
    def _(j):
        pltpu.make_async_copy(
            a_hbm.at[:, pl.ds(pl.multiple_of(j * (rep_n * BLK) + (r // 2) * 128, 128), 128)],
            ab.at[j], sem_ab).start()

    barrier = pltpu.get_barrier_semaphore()
    for peer in peers:
        pl.semaphore_signal(barrier, inc=1, device_id=peer, device_id_type=pl.DeviceIdType.MESH)

    own = pl.ds(pl.multiple_of((i * ZN + z) * BLK, BLK), BLK)
    xg[own, :] = x_ref[...]
    w2p[...] = jnp.zeros_like(w2p)
    w2p[:, :classes] = w2_ref[...].astype(BF)
    mask_row = msk_ref[...].astype(F32)
    mt[...] = jnp.broadcast_to(jnp.sum(mask_row, axis=1, keepdims=True), mt.shape)
    pl.semaphore_wait(barrier, len(peers))

    pending = []

    def send(src, dst, ssem, rsem, device):
        cp = pltpu.make_async_remote_copy(src_ref=src, dst_ref=dst, send_sem=ssem, recv_sem=rsem,
                                          device_id=device, device_id_type=pl.DeviceIdType.MESH)
        cp.start()
        pending.append(cp)
        return cp

    def gather(g, slot, axis_n, axis_order, peer_of, me, fillers=()):
        fillers = list(fillers)
        zc = {d: send(slot(z, me), slot(z, me), zs.at[g, d], zrv.at[g, d], dev(dz=d)) for d in z_order}
        axc = {}

        def spread(zk, k):
            for e in axis_order:
                axc[k, e] = send(slot(zk, me), slot(zk, me), as_.at[g, k, e], arv.at[g, k, e], peer_of(e))

        spread(z, 0)
        for d in z_order:
            if fillers:
                fillers.pop(0)()
            zc[d].wait_recv()
            spread(lax.rem(z + ZN - d, ZN), d)
        while fillers:
            fillers.pop(0)()
        return axc

    def exchange_small(k, src, buf, order, peer_of):
        return [send(src, buf.at[e], ms.at[k, e], mrv.at[k, e], peer_of(e)) for e in order]

    def compress():
        pltpu.make_async_copy(af, af, sem_af).wait()

        @pl.loop(0, n_q // 2)
        def _(p):
            even = af[:, pl.ds(pl.multiple_of(p * 256, 256), 128)]
            odd = af[:, pl.ds(pl.multiple_of(p * 256 + 128, 128), 128)]
            out = pl.ds(pl.multiple_of(p * 128, 128), 128)

            @pl.when(lax.rem(y, 2) == 0)
            def _():
                ac[:, out] = jnp.concatenate([even[:, :BLK], odd[:, :BLK]], axis=1)

            @pl.when(lax.rem(y, 2) == 1)
            def _():
                ac[:, out] = jnp.concatenate([even[:, BLK:], odd[:, BLK:]], axis=1)

    def transpose_part(lo, hi):
        def run():
            @pl.loop(lo, hi)
            def _(j):
                src_j = lax.rem(j, XN) * 2 + j // XN
                t = ab[src_j].T
                rows = pl.ds(pl.multiple_of(j * BLK, BLK), BLK)

                @pl.when(lax.rem(r, 2) == 0)
                def _():
                    at[rows, :] = t[:BLK]

                @pl.when(lax.rem(r, 2) == 1)
                def _():
                    at[rows, :] = t[BLK:]
        return run

    def wait_ab():
        pltpu.make_async_copy(ab, ab, sem_ab).wait()

    fill = [compress, wait_ab] + [transpose_part(k, k + 1) for k in range(node_n)]

    def fwd_gather(g, buf, fillers=()):
        def slot(zk, xk):
            return buf.at[pl.ds(pl.multiple_of(((xk * 2 + c) * ZN + zk) * BLK, BLK), BLK), :]

        axc = gather(g, slot, XN, x_order, lambda e: dev(dx_=e), x, fillers)
        core = []

        def line(xk):
            return buf.at[pl.ds(pl.multiple_of((xk * 2 + c) * ZN * BLK, ZN * BLK), ZN * BLK), :]

        core.append(send(line(x), line(x), cs.at[g, 0], crv.at[g, 0], dev(dc=1)))
        for e in x_order:
            for k in [0] + z_order:
                axc[k, e].wait_recv()
            xk = lax.rem(x + XN - e, XN)
            core.append(send(line(xk), line(xk), cs.at[g, e], crv.at[g, e], dev(dc=1)))
        for cp in core:
            cp.wait_recv()

    def fwd_reduce(g, buf):
        part = jnp.dot(ac[...], buf[...], preferred_element_type=F32)
        for k in range(YN):
            zp[g, k] = part[k * BLK:(k + 1) * BLK]
        cps = [send(zp.at[g, lax.rem(y + e, YN)], zr.at[g, e], rs.at[g, e], rrv.at[g, e], dev(dy=e)) for e in y_order]
        total = zp[g, y]
        for e, cp in zip(y_order, cps):
            cp.wait_recv()
            total = total + zr[g, e]
        return total

    mzc = exchange_small(0, mt.at[0], mz, z_order, lambda e: dev(dz=e))
    fwd_gather(0, xg, fill)
    b1 = w1_ref[...].astype(BF)
    chunk = min(512, xg.shape[0])

    @pl.loop(0, xg.shape[0] // chunk)
    def _(k):
        rows = pl.ds(pl.multiple_of(k * chunk, chunk), chunk)
        yg[rows, :] = jnp.dot(xg[rows, :], b1, preferred_element_type=F32).astype(BF)

    def small_sum(k, cps, order, buf, nxt):
        s = mt[k]
        for e, cp in zip(order, cps):
            cp.wait_recv()
            s = s + buf[e]
        mt[nxt] = s

    small_sum(0, mzc, z_order, mz, 1)
    mxc = exchange_small(1, mt.at[1], mx, x_order, lambda e: dev(dx_=e))
    z1 = fwd_reduce(0, yg)
    z1s[...] = z1
    h1 = jnp.maximum(z1, 0.0).astype(BF)
    h1s[...] = h1
    small_sum(1, mxc, x_order, mx, 2)
    myc = exchange_small(2, mt.at[2], my, y_order, lambda e: dev(dy=e))

    y2g[own, :] = jnp.dot(h1, w2p[...], preferred_element_type=F32).astype(BF)
    fwd_gather(1, y2g)
    small_sum(2, myc, y_order, my, 3)
    mcc = exchange_small(3, mt.at[3], mc, [1], lambda e: dev(dc=e))
    z2 = fwd_reduce(1, y2g)
    small_sum(3, mcc, [1], mc, 4)

    count = mt[4][:1, :1]
    diag = lax.broadcasted_iota(jnp.int32, (BLK, BLK), 0) == lax.broadcasted_iota(jnp.int32, (BLK, BLK), 1)
    labf = jnp.sum(jnp.where(diag, jnp.broadcast_to(lab_ref[...].astype(F32), (BLK, BLK)), 0.0), axis=1, keepdims=True)
    mskf = jnp.sum(jnp.where(diag, jnp.broadcast_to(mask_row, (BLK, BLK)), 0.0), axis=1, keepdims=True)
    lane = lax.broadcasted_iota(jnp.int32, z2.shape, 1)
    logits = jnp.where(lane < classes, z2, NEG)
    shifted = logits - jnp.max(logits, axis=1, keepdims=True)
    log_probs = shifted - jnp.log(jnp.sum(jnp.exp(shifted), axis=1, keepdims=True))
    onehot = jnp.where(lane.astype(F32) == labf, 1.0, 0.0)
    local_loss = -jnp.sum(mskf * jnp.sum(onehot * log_probs, axis=1, keepdims=True), axis=0, keepdims=True)
    g2 = ((jnp.exp(log_probs) - onehot) * (mskf / count)).astype(BF)

    def bwd(g, buf, value):
        def slot(zk, yk):
            return buf.at[pl.ds(pl.multiple_of((zk * YN + yk) * BLK, BLK), BLK), :]

        buf[pl.ds(pl.multiple_of(r * BLK, BLK), BLK), :] = value
        axc = gather(g, slot, YN, y_order, lambda e: dev(dy=e), y)
        for cp in axc.values():
            cp.wait_recv()
        b = g - 2
        part = jnp.dot(at[...], buf[...], preferred_element_type=F32)
        half = XN * BLK
        dp[b, 0] = part[:half]
        dp[b, 1] = part[half:]
        cp = send(dp.at[b, 1 - c], dr.at[b], cs.at[g, 0], crv.at[g, 0], dev(dc=1))
        cp.wait_recv()
        ds_[b] = dp[b, c] + dr[b]

        def mine(xk):
            return pl.ds(pl.multiple_of(xk * BLK, BLK), BLK)

        cps = [send(ds_.at[b, mine(lax.rem(x + e, XN))], dx.at[b, e], rs.at[g, e], rrv.at[g, e], dev(dx_=e)) for e in x_order]
        total = ds_[b, mine(x)]
        for e, cp in zip(x_order, cps):
            cp.wait_recv()
            total = total + dx[b, e]
        return total.astype(BF)

    d2 = bwd(2, g2g, g2)
    tdims = (((0,), (0,)), ((), ()))
    dw2 = lax.dot_general(h1s[...], d2, tdims, preferred_element_type=F32)
    dh1 = lax.dot_general(d2, w2p[...], (((1,), (1,)), ((), ())), preferred_element_type=F32)
    g1 = jnp.where(z1s[...] > 0, dh1, 0.0).astype(BF)
    d1 = bwd(3, g1g, g1)
    dw1 = lax.dot_general(x_ref[...], d1, tdims, preferred_element_type=F32)

    f_in = x_ref.shape[1]
    pay[0:f_in] = dw1[:, :128]
    pay[f_in:2 * f_in] = dw1[:, 128:]
    o2 = 2 * f_in
    pay[o2:o2 + hidden] = dw2[:, :128]
    row = lax.broadcasted_iota(jnp.int32, (hidden, 128), 0)
    lane2 = lax.broadcasted_iota(jnp.int32, (hidden, 128), 1)
    pay[o2 + hidden:o2 + 2 * hidden] = jnp.where(jnp.logical_and(row == 0, lane2 == 127), local_loss, dw2[:, 128:])
    n_rows = o2 + 2 * hidden
    rx = n_rows // node_n
    ry = rx // YN
    half = XN * rx

    cp = send(pay.at[pl.ds(pl.multiple_of((1 - c) * half, 8), half)], payd, fs.at[0, 0], frv.at[0, 0], dev(dc=1))
    cp.wait_recv()
    payd[...] = payd[...] + pay[pl.ds(pl.multiple_of(c * half, 8), half)]
    cps = [send(payd.at[pl.ds(pl.multiple_of(lax.rem(x + e, XN) * rx, 8), rx)], payx.at[e], fs.at[1, e], frv.at[1, e], dev(dx_=e)) for e in x_order]
    s = payd[pl.ds(pl.multiple_of(x * rx, 8), rx)]
    for e, cp in zip(x_order, cps):
        cp.wait_recv()
        s = s + payx[e]
    payx[0] = s
    cps = [send(payx.at[0, pl.ds(pl.multiple_of(lax.rem(y + e, YN) * ry, 8), ry)], payy.at[e], fs.at[2, e], frv.at[2, e], dev(dy=e)) for e in y_order]
    s = payx[0, pl.ds(pl.multiple_of(y * ry, 8), ry)]
    for e, cp in zip(y_order, cps):
        cp.wait_recv()
        s = s + payy[e]
    payz[z] = s
    cps = [send(payz.at[z], payz.at[z], fs.at[3, d], frv.at[3, d], dev(dz=d)) for d in z_order]
    for cp in cps:
        cp.wait_recv()
    s = payz[0]
    for k in range(1, ZN):
        s = s + payz[k]
    out = pay
    base = (c * XN + x) * rx
    for cp in pending:
        cp.wait_send()
    pending.clear()
    fin = af_out = ds_out = None
    fin = y2pad
    fin[pl.ds(pl.multiple_of(base + y * ry, 8), ry)] = s
    mine = fin.at[pl.ds(pl.multiple_of(base + y * ry, 8), ry)]
    cps = [send(mine, mine, fs.at[4, e], frv.at[4, e], dev(dy=e)) for e in y_order]
    for cp in cps:
        cp.wait_recv()
    mine = fin.at[pl.ds(pl.multiple_of(base, 8), rx)]
    cps = [send(mine, mine, fs.at[5, e], frv.at[5, e], dev(dx_=e)) for e in x_order]
    for cp in cps:
        cp.wait_recv()
    mine = fin.at[pl.ds(pl.multiple_of(c * half, 8), half)]
    cp = send(mine, mine, fs.at[6, 0], frv.at[6, 0], dev(dc=1))
    cp.wait_recv()
    dw1_ref[:, :128] = fin[0:f_in]
    dw1_ref[:, 128:] = fin[f_in:2 * f_in]
    dw2_ref[:, :128] = fin[o2:o2 + hidden]
    tail = fin[o2 + hidden:o2 + 2 * hidden]
    dw2_ref[:, 128:] = tail[:, :classes - 128]
    loss_ref[0, 0] = jnp.sum(tail[:1, 127:] / count)
    for cp in pending:
        cp.wait_send()


def solution(mesh):
    rep_n, node_n = mesh.shape["rep"], mesh.shape["nodes"]
    YN = 4 if rep_n == 32 else 2
    ZN = rep_n // YN
    XN = node_n // 2

    def local_step(adj, features, w_one, w_two, labels, mask):
        f_in, hidden = w_one.shape
        classes = w_two.shape[1]
        rows_g = adj.shape[0]
        cols_y = node_n * ZN * BLK
        n_pay = 2 * f_in + 2 * hidden
        rx = n_pay // node_n
        V = pltpu.VMEM
        D = pltpu.SemaphoreType.DMA
        scratch = dict(
            af=V((YN * BLK, node_n * ZN * 128), BF), ac=V((YN * BLK, cols_y), BF),
            ab=V((node_n, rows_g, 128), BF), at=V((node_n * BLK, rows_g), BF),
            xg=V((cols_y, f_in), BF), yg=V((cols_y, hidden), BF), y2g=V((cols_y, 256), BF),
            g2g=V((rows_g, 256), BF), g1g=V((rows_g, hidden), BF),
            zp=V((2, YN, BLK, 256), F32), zr=V((2, YN, BLK, 256), F32),
            dp=V((2, 2, XN * BLK, 256), F32), dr=V((2, XN * BLK, 256), F32), ds_=V((2, XN * BLK, 256), F32),
            dx=V((2, XN, BLK, 256), F32),
            pay=V((n_pay, 128), F32), payd=V((n_pay // 2, 128), F32), payx=V((XN, rx, 128), F32),
            payy=V((YN, rx // YN, 128), F32), payz=V((ZN, rx // YN, 128), F32),
            mt=V((5, 8, 128), F32), mz=V((ZN, 8, 128), F32), mx=V((XN, 8, 128), F32), my=V((YN, 8, 128), F32),
            mc=V((2, 8, 128), F32),
            z1s=V((BLK, hidden), F32), h1s=V((BLK, hidden), BF), y2pad=V((n_pay, 128), F32), w2p=V((hidden, 256), BF),
            sem_af=D, sem_ab=D,
            zs=D((4, ZN)), zrv=D((4, ZN)), as_=D((4, ZN, 4)), arv=D((4, ZN, 4)), cs=D((4, 4)), crv=D((4, 4)),
            rs=D((4, 4)), rrv=D((4, 4)), ms=D((4, ZN)), mrv=D((4, ZN)), fs=D((7, ZN)), frv=D((7, ZN)),
        )
        vm = pl.BlockSpec(memory_space=pltpu.VMEM)
        loss, dw1, dw2 = pl.pallas_call(
            functools.partial(step_kernel, ZN, YN, XN),
            out_shape=(jax.ShapeDtypeStruct((1, 1), F32), jax.ShapeDtypeStruct((f_in, hidden), F32),
                       jax.ShapeDtypeStruct((hidden, classes), F32)),
            in_specs=[pl.BlockSpec(memory_space=pl.ANY), vm, vm, vm, vm, vm],
            out_specs=(pl.BlockSpec(memory_space=pltpu.SMEM), vm, vm),
            scratch_shapes=list(scratch.values()),
            compiler_params=pltpu.CompilerParams(collective_id=0, has_side_effects=True, vmem_limit_bytes=60 * 2 ** 20),
            name="gcn_step",
        )(adj, features, w_one, w_two, labels.reshape(1, BLK), mask.reshape(1, BLK))
        return loss.reshape(()), dw1, dw2

    row_spec = P(("nodes", "rep"))
    return jax.shard_map(local_step, mesh=mesh, in_specs=(P("nodes", None), P(("nodes", "rep"), None), P(), P(), row_spec, row_spec),
                         out_specs=(P(), P(), P()), check_vma=False)
```

```python
import functools

import jax
import jax.numpy as jnp
from jax import lax
from jax.experimental import pallas as pl
from jax.experimental.pallas import tpu as pltpu
from jax.sharding import PartitionSpec as P

BF = jnp.bfloat16
F32 = jnp.float32
BLK = 64
NEG = -1e30


def ring_order(n):
    return sorted(range(1, n), key=lambda d: (min(d, n - d), d))


def pack(v):
    out = []
    lane = lax.broadcasted_iota(jnp.int32, (BLK // 2, 128), 1)
    for k in range(v.shape[0] // BLK):
        lo, hi = v[k * BLK:(k + 1) * BLK, :128], v[k * BLK:(k + 1) * BLK, 128:]
        out += [lo, jnp.where(lane < 64, hi[:BLK // 2], pltpu.roll(hi[BLK // 2:], 64, 1))]
    return jnp.concatenate(out, axis=0)


def unpack(p):
    lane = lax.broadcasted_iota(jnp.int32, (BLK // 2, 128), 1)
    t = p[BLK:]
    hi = jnp.concatenate([jnp.where(lane < 64, t, 0.0), jnp.where(lane < 64, pltpu.roll(t, 64, 1), 0.0)], axis=0)
    return jnp.concatenate([p[:BLK], hi], axis=1)


def step_kernel(ZN, YN, XN, names, *refs):
    R = dict(zip(names, refs))
    a_hbm, x_ref, w1_ref, w2_ref = R["a"], R["x"], R["w1"], R["w2"]
    af, ac, ab, at, w2p, mt = R["af"], R["ac"], R["ab"], R["at"], R["w2p"], R["mt"]
    rep_n, node_n = ZN * YN, 2 * XN
    r, i = lax.axis_index("rep"), lax.axis_index("nodes")
    z, y = r // YN, lax.rem(r, YN)
    x, c = i // 2, lax.rem(i, 2)
    classes, hidden = w2_ref.shape
    f_in = x_ref.shape[1]
    PB = 96

    def dev(dz=0, dy=0, dx=0, dc=0):
        return {"rep": lax.rem(z + dz, ZN) * YN + lax.rem(y + dy, YN),
                "nodes": lax.rem(x + dx, XN) * 2 + lax.rem(c + dc, 2)}

    def rows(k, n):
        return pl.ds(pl.multiple_of(k * n, n), n)

    z_order, y_order, x_order = ring_order(ZN), ring_order(YN), ring_order(XN)
    peers = [dev(dz=d) for d in z_order] + [dev(dy=d) for d in y_order] + [dev(dx=d) for d in x_order] + [dev(dc=1)]

    rows_z = YN * BLK
    n_q = node_n * ZN

    @pl.loop(0, n_q)
    def _(q):
        pltpu.make_async_copy(
            a_hbm.at[rows(z, rows_z), pl.ds(pl.multiple_of(q * (YN * BLK) + (y // 2) * 128, 128), 128)],
            af.at[:, rows(q, 128)], R["sem_af"]).start()

    @pl.loop(0, node_n)
    def _(j):
        pltpu.make_async_copy(
            a_hbm.at[:, pl.ds(pl.multiple_of(j * (rep_n * BLK) + (r // 2) * 128, 128), 128)],
            ab.at[j], R["sem_ab"]).start()

    barrier = pltpu.get_barrier_semaphore()
    for peer in peers:
        pl.semaphore_signal(barrier, inc=1, device_id=peer, device_id_type=pl.DeviceIdType.MESH)

    xg, yg, y2g, g2g, g1g = R["xg"], R["yg"], R["y2g"], R["g2g"], R["g1g"]
    own_f = (c * ZN + z) * XN + x
    xg[rows(own_f, BLK), :] = x_ref[...]
    w2p[...] = jnp.zeros_like(w2p)
    w2p[:classes, :] = w2_ref[...].astype(BF)
    b1 = w1_ref[...].astype(BF)
    mask_row = R["msk"][...].astype(F32)
    mt[0] = jnp.broadcast_to(jnp.sum(mask_row, axis=1, keepdims=True), mt.shape[1:])

    pltpu.make_async_copy(af, af, R["sem_af"]).wait()

    @pl.loop(0, n_q // 2)
    def _(p):
        xp = lax.rem(p, XN // 2)
        zk = lax.rem(p // (XN // 2), ZN)
        ck = p // (XN // 2 * ZN)
        q = (4 * xp + ck) * ZN + zk
        even, odd = af[:, rows(q, 128)], af[:, rows(q + 2 * ZN, 128)]
        out = rows(p, 128)

        @pl.when(lax.rem(y, 2) == 0)
        def _():
            ac[:, out] = jnp.concatenate([even[:, :BLK], odd[:, :BLK]], axis=1)

        @pl.when(lax.rem(y, 2) == 1)
        def _():
            ac[:, out] = jnp.concatenate([even[:, BLK:], odd[:, BLK:]], axis=1)

    pl.semaphore_wait(barrier, len(peers))

    pending = []

    def send(src, dst, ssem, rsem, device):
        cp = pltpu.make_async_remote_copy(src_ref=src, dst_ref=dst, send_sem=ssem, recv_sem=rsem,
                                          device_id=device, device_id_type=pl.DeviceIdType.MESH)
        cp.start()
        pending.append(cp)
        return cp

    def gather(g, buf, index, size, n, me, peer_of, done, fillers=()):
        fillers = list(fillers)
        half = size // 2
        zs, zr, ss, sr = R["zs"], R["zr"], R["ss"], R["sr"]

        def slot(zk, ak):
            return buf.at[rows(index(zk, ak), size)]

        def part(zk, ak, h):
            return buf.at[pl.ds(pl.multiple_of(index(zk, ak) * size + h * half, half), half)]

        def zof(k):
            return lax.rem(z + ZN - k, ZN)

        order = [0] + z_order
        zc = {d: send(slot(z, me), slot(z, me), zs.at[g, d], zr.at[g, d], dev(dz=d)) for d in z_order}
        near, far = {}, {}

        def spread(k):
            mine = slot(zof(k), me)
            near[k] = [send(mine, mine, ss.at[g, k, e], sr.at[g, k, e], peer_of(e)) for e in ([1, 3] if n == 4 else [1])]

        def relay(k):
            far[k] = []
            for h, cp in enumerate(near[k]):
                cp.wait_recv()
                if n == 4:
                    piece = part(zof(k), lax.rem(me + (3 if h == 0 else 1), n), h)
                    far[k].append(send(piece, piece, ss.at[g, k, 2 * h], sr.at[g, k, 2 * h], peer_of(1 if h == 0 else 3)))

        def finish(k):
            for cp in far[k]:
                cp.wait_recv()
            done(zof(k), k)

        steps = len(order)
        for s in range(steps + 2):
            if s < steps:
                if s:
                    if fillers:
                        fillers.pop(0)()
                    zc[order[s]].wait_recv()
                spread(order[s])
            if 1 <= s <= steps:
                relay(order[s - 1])
            if s >= 2:
                finish(order[s - 2])
        while fillers:
            fillers.pop(0)()

    def transpose_part(j):
        def run():
            if j == 0:
                pltpu.make_async_copy(ab, ab, R["sem_ab"]).wait()
            t = ab[(j % XN) * 2 + j // XN].T

            @pl.when(lax.rem(r, 2) == 0)
            def _():
                at[j * BLK:(j + 1) * BLK, :] = t[:BLK]

            @pl.when(lax.rem(r, 2) == 1)
            def _():
                at[j * BLK:(j + 1) * BLK, :] = t[BLK:]
        return run

    fill = [transpose_part(j) for j in range(node_n)]

    def unpack_rows(buf, first_block, n, out):
        for k in range(n):
            base = pl.multiple_of((first_block + k) * PB, 32)
            orow = pl.multiple_of((first_block + k) * BLK, BLK)
            t = buf[pl.ds(base + BLK, BLK // 2), :]
            out[pl.ds(orow, BLK), :128] = buf[pl.ds(base, BLK), :]
            out[pl.ds(orow, BLK // 2), 128:] = t
            out[pl.ds(orow + BLK // 2, BLK // 2), 128:] = jnp.concatenate([t[:, 64:], t[:, :64]], axis=1)

    zacc = R["zacc"]

    def fwd_gather(g, buf, size, prepare, fillers=()):
        late = []

        def line(ck, zk):
            return buf.at[rows(ck * ZN + zk, XN * size)]

        def add(ck, zk, first):
            k = ck * ZN + zk
            prepare(k)
            v = jnp.dot(ac[:, rows(k, XN * BLK)], yg[g, rows(k, XN * BLK), :], preferred_element_type=F32)
            if first:
                zacc[...] = v
            else:
                zacc[...] += v

        def partner():
            cp, zk = late.pop(0)
            cp.wait_recv()
            add(1 - c, zk, False)

        def done(zk, k):
            mine = line(c, zk)
            late.append((send(mine, mine, R["cs"].at[g, k], R["cr"].at[g, k], dev(dc=1)), zk))
            add(c, zk, k == 0)
            if len(late) > 1:
                partner()

        gather(g, buf, lambda zk, xk: (c * ZN + zk) * XN + xk, size, XN, x, lambda e: dev(dx=e), done, fillers)
        while late:
            partner()

    def fwd_reduce(g, packed):
        zp, zr = (R["zpp"], R["zrp"]) if packed else (R["zp"], R["zrw"])
        v = zacc[...]
        for k in range(YN):
            piece = v[k * BLK:(k + 1) * BLK]
            zp[k] = pack(piece) if packed else piece
        cps = [send(zp.at[lax.rem(y + e, YN)], zr.at[e], R["rs"].at[g, e], R["rr"].at[g, e], dev(dy=e)) for e in y_order]
        total = zp[y]
        for e, cp in zip(y_order, cps):
            cp.wait_recv()
            total = total + zr[e]
        return unpack(total) if packed else total

    def exchange_small(k, src, buf, order, peer_of):
        return [send(src, buf.at[e], R["ms"].at[k, e], R["mr"].at[k, e], peer_of(e)) for e in order]

    def small_sum(k, cps, order, buf, nxt):
        s = mt[k]
        for e, cp in zip(order, cps):
            cp.wait_recv()
            s = s + buf[e]
        mt[nxt] = s

    def y1_rows(k):
        rr = rows(k, XN * BLK)
        yg[0, rr, :] = jnp.dot(xg[rr, :], b1, preferred_element_type=F32).astype(BF)

    def y2_rows(k):
        unpack_rows(y2g, k * XN, XN, yg.at[1])

    mzc = exchange_small(0, mt.at[0], R["mz"], z_order, lambda e: dev(dz=e))
    fwd_gather(0, xg, BLK, y1_rows, fill[:node_n // 2])
    small_sum(0, mzc, z_order, R["mz"], 1)
    mxc = exchange_small(1, mt.at[1], R["mx"], x_order, lambda e: dev(dx=e))
    z1 = fwd_reduce(0, False)
    R["z1s"][...] = z1
    h1 = jnp.maximum(z1, 0.0).astype(BF)
    R["h1s"][...] = h1
    nt = (((1,), (1,)), ((), ()))
    y2 = lax.dot_general(h1, w2p[...], nt, preferred_element_type=F32)
    y2g[rows(own_f, PB), :] = pack(y2).astype(BF)
    small_sum(1, mxc, x_order, R["mx"], 2)
    myc = exchange_small(2, mt.at[2], R["my"], y_order, lambda e: dev(dy=e))
    fwd_gather(1, y2g, PB, y2_rows, fill[node_n // 2:])
    small_sum(2, myc, y_order, R["my"], 3)
    mcc = exchange_small(3, mt.at[3], R["mc"], [1], lambda e: dev(dc=e))
    z2 = fwd_reduce(1, True)
    small_sum(3, mcc, [1], R["mc"], 4)

    count = mt[4][:1, :1]
    diag = lax.broadcasted_iota(jnp.int32, (BLK, BLK), 0) == lax.broadcasted_iota(jnp.int32, (BLK, BLK), 1)
    labf = jnp.sum(jnp.where(diag, jnp.broadcast_to(R["lab"][...].astype(F32), (BLK, BLK)), 0.0), axis=1, keepdims=True)
    mskf = jnp.sum(jnp.where(diag, jnp.broadcast_to(mask_row, (BLK, BLK)), 0.0), axis=1, keepdims=True)
    lane = lax.broadcasted_iota(jnp.int32, z2.shape, 1)
    logits = jnp.where(lane < classes, z2, NEG)
    shifted = logits - jnp.max(logits, axis=1, keepdims=True)
    log_probs = shifted - jnp.log(jnp.sum(jnp.exp(shifted), axis=1, keepdims=True))
    onehot = jnp.where(lane.astype(F32) == labf, 1.0, 0.0)
    g2 = (jnp.exp(log_probs) - onehot) * (mskf / count)
    g2g[rows(r, PB), :] = pack(g2).astype(BF)
    local_loss = -jnp.sum(mskf * jnp.sum(onehot * log_probs, axis=1, keepdims=True), axis=0, keepdims=True)

    dacc = R["dacc"]

    def bwd(g, buf, size, packed, fillers=()):
        gu = R["gu"] if packed else buf

        def done(zk, k):
            if packed:
                unpack_rows(buf, zk * YN, YN, gu)
            rr = rows(zk, YN * BLK)
            v = jnp.dot(at[:, rr], gu[rr, :], preferred_element_type=F32)
            if k == 0:
                dacc[...] = v
            else:
                dacc[...] += v

        gather(g, buf, lambda zk, yk: zk * YN + yk, size, YN, y, lambda e: dev(dy=e), done, fillers)
        dp, dr, dsum, dx = (R["dpp"], R["drp"], R["dsp"], R["dxp"]) if packed else (R["dp"], R["dr"], R["ds"], R["dx"])
        for k in range(2):
            for j in range(XN):
                piece = dacc[(k * XN + j) * BLK:(k * XN + j + 1) * BLK]
                dp[k, j] = pack(piece) if packed else piece
        cp = send(dp.at[1 - c], dr, R["cs"].at[g, 0], R["cr"].at[g, 0], dev(dc=1))
        cp.wait_recv()
        dsum[...] = dp[c] + dr[...]
        cps = [send(dsum.at[lax.rem(x + e, XN)], dx.at[e], R["rs"].at[g, e], R["rr"].at[g, e], dev(dx=e)) for e in x_order]
        total = dsum[x]
        for e, cp in zip(x_order, cps):
            cp.wait_recv()
            total = total + dx[e]
        return (unpack(total) if packed else total).astype(BF)

    def all_reduce(t, pay, payd, payx, payy, payz, fin):
        n_rows = pay.shape[0]
        rx = n_rows // node_n
        ry = rx // YN
        half = XN * rx
        fs, fr = R["fs"], R["fr"]
        state = {}
        base = (c * XN + x) * rx

        def s0():
            state["cp"] = [send(pay.at[rows(1 - c, half)], payd, fs.at[t, 0, 0], fr.at[t, 0, 0], dev(dc=1))]

        def s1():
            state["cp"][0].wait_recv()
            payd[...] = payd[...] + pay[rows(c, half)]
            state["cp"] = [send(payd.at[rows(lax.rem(x + e, XN), rx)], payx.at[e], fs.at[t, 1, e], fr.at[t, 1, e], dev(dx=e)) for e in x_order]

        def s2():
            s = payd[rows(x, rx)]
            for e, cp in zip(x_order, state["cp"]):
                cp.wait_recv()
                s = s + payx[e]
            payx[0] = s
            state["cp"] = [send(payx.at[0, rows(lax.rem(y + e, YN), ry)], payy.at[e], fs.at[t, 2, e], fr.at[t, 2, e], dev(dy=e)) for e in y_order]

        def s3():
            s = payx[0, rows(y, ry)]
            for e, cp in zip(y_order, state["cp"]):
                cp.wait_recv()
                s = s + payy[e]
            payz[z] = s
            state["cp"] = [send(payz.at[z], payz.at[z], fs.at[t, 3, d], fr.at[t, 3, d], dev(dz=d)) for d in z_order]

        def s4():
            for cp in state["cp"]:
                cp.wait_recv()
            s = payz[0]
            for k in range(1, ZN):
                s = s + payz[k]
            mine = fin.at[pl.ds(pl.multiple_of(base + y * ry, 8), ry)]
            fin[pl.ds(pl.multiple_of(base + y * ry, 8), ry)] = s
            state["cp"] = [send(mine, mine, fs.at[t, 4, e], fr.at[t, 4, e], dev(dy=e)) for e in y_order]

        def s5():
            for cp in state["cp"]:
                cp.wait_recv()
            mine = fin.at[pl.ds(pl.multiple_of(base, 8), rx)]
            state["cp"] = [send(mine, mine, fs.at[t, 5, e], fr.at[t, 5, e], dev(dx=e)) for e in x_order]

        def s6():
            for cp in state["cp"]:
                cp.wait_recv()
            mine = fin.at[rows(c, half)]
            state["cp"] = [send(mine, mine, fs.at[t, 6, 0], fr.at[t, 6, 0], dev(dc=1))]

        def s7():
            state["cp"][0].wait_recv()

        return [s0, s1, s2, s3, s4, s5, s6, s7]

    d2 = bwd(2, g2g, PB, True)
    tn = (((0,), (0,)), ((), ()))
    dh1 = jnp.dot(d2, w2p[...], preferred_element_type=F32)
    g1g[rows(r, BLK), :] = jnp.where(R["z1s"][...] > 0, dh1, 0.0).astype(BF)
    R["d2s"][...] = d2
    ar2 = all_reduce(0, R["pay2"], R["payd2"], R["payx2"], R["payy2"], R["payz2"], R["fin2"])

    def make_dw2():
        dw2 = lax.dot_general(R["d2s"][...], R["h1s"][...], tn, preferred_element_type=F32)
        row = lax.broadcasted_iota(jnp.int32, (256, 128), 0)
        lane2 = lax.broadcasted_iota(jnp.int32, (256, 128), 1)
        R["pay2"][0:256] = jnp.where(jnp.logical_and(row == 255, lane2 == 127), local_loss, dw2[:, :128])
        R["pay2"][256:512] = dw2[:, 128:]
        ar2[0]()

    def nothing():
        pass

    d1 = bwd(3, g1g, BLK, False, [make_dw2, nothing, ar2[1], nothing, ar2[2], nothing, ar2[3]])
    dw1 = lax.dot_general(x_ref[...], d1, tn, preferred_element_type=F32)
    R["pay1"][0:f_in] = dw1[:, :128]
    R["pay1"][f_in:2 * f_in] = dw1[:, 128:]
    ar1 = all_reduce(1, R["pay1"], R["payd1"], R["payx1"], R["payy1"], R["payz1"], R["fin1"])
    for s in range(8):
        ar1[s]()
        if s < 4:
            ar2[4 + s]()
    fin1, fin2 = R["fin1"], R["fin2"]
    R["dw2"][:, :128] = fin2[0:classes]
    R["dw2"][:, 128:] = fin2[256:256 + classes]
    R["loss"][0, 0] = jnp.sum(fin2[255:256, 127:] / count)
    R["dw1"][:, :128] = fin1[0:f_in]
    R["dw1"][:, 128:] = fin1[f_in:2 * f_in]
    for cp in pending:
        cp.wait_send()


def solution(mesh):
    rep_n, node_n = mesh.shape["rep"], mesh.shape["nodes"]
    YN = 4
    ZN = rep_n // YN
    XN = node_n // 2

    def local_step(adj, features, w_one, w_two, labels, mask):
        f_in, hidden = w_one.shape
        classes = w_two.shape[1]
        rows_g = adj.shape[0]
        blocks_y = node_n * ZN
        V = pltpu.VMEM
        D = pltpu.SemaphoreType.DMA

        def reduce_bufs(t, n):
            rx = n // node_n
            return {f"pay{t}": V((n, 128), F32), f"payd{t}": V((n // 2, 128), F32), f"payx{t}": V((XN, rx, 128), F32),
                    f"payy{t}": V((YN, rx // YN, 128), F32), f"payz{t}": V((ZN, rx // YN, 128), F32), f"fin{t}": V((n, 128), F32)}

        scratch = dict(
            af=V((YN * BLK, blocks_y * 128), BF), ac=V((YN * BLK, blocks_y * BLK), BF),
            ab=V((node_n, rows_g, 128), BF), at=V((node_n * BLK, rows_g), BF),
            xg=V((blocks_y * BLK, f_in), BF), yg=V((2, blocks_y * BLK, 256), BF), y2g=V((blocks_y * 96, 128), BF),
            g2g=V((rep_n * 96, 128), BF), gu=V((rows_g, 256), BF), g1g=V((rows_g, hidden), BF),
            zacc=V((YN * BLK, 256), F32), dacc=V((node_n * BLK, 256), F32),
            zp=V((YN, BLK, 256), F32), zrw=V((YN, BLK, 256), F32), zpp=V((YN, 96, 128), F32), zrp=V((YN, 96, 128), F32),
            dp=V((2, XN, BLK, 256), F32), dr=V((XN, BLK, 256), F32), ds=V((XN, BLK, 256), F32), dx=V((XN, BLK, 256), F32),
            dpp=V((2, XN, 96, 128), F32), drp=V((XN, 96, 128), F32), dsp=V((XN, 96, 128), F32), dxp=V((XN, 96, 128), F32),
            mt=V((5, 8, 128), F32), mz=V((ZN, 8, 128), F32), mx=V((XN, 8, 128), F32), my=V((YN, 8, 128), F32),
            mc=V((2, 8, 128), F32),
            z1s=V((BLK, hidden), F32), h1s=V((BLK, hidden), BF), d2s=V((BLK, 256), BF), w2p=V((256, hidden), BF),
            sem_af=D, sem_ab=D,
            zs=D((4, 8)), zr=D((4, 8)), ss=D((4, 8, 4)), sr=D((4, 8, 4)), cs=D((4, 8)), cr=D((4, 8)),
            rs=D((4, 4)), rr=D((4, 4)), ms=D((4, 8)), mr=D((4, 8)), fs=D((2, 7, 8)), fr=D((2, 7, 8)),
        )
        scratch.update(reduce_bufs(1, 2 * f_in))
        scratch.update(reduce_bufs(2, 512))
        names = ["a", "x", "w1", "w2", "lab", "msk", "loss", "dw1", "dw2"] + list(scratch)
        vm = pl.BlockSpec(memory_space=pltpu.VMEM)
        loss, dw1, dw2 = pl.pallas_call(
            functools.partial(step_kernel, ZN, YN, XN, names),
            out_shape=(jax.ShapeDtypeStruct((1, 1), F32), jax.ShapeDtypeStruct((f_in, hidden), F32),
                       jax.ShapeDtypeStruct((classes, hidden), F32)),
            in_specs=[pl.BlockSpec(memory_space=pl.ANY), vm, vm, vm, vm, vm],
            out_specs=(pl.BlockSpec(memory_space=pltpu.SMEM), vm, vm),
            scratch_shapes=list(scratch.values()),
            compiler_params=pltpu.CompilerParams(collective_id=0, has_side_effects=True, vmem_limit_bytes=60 * 2 ** 20),
            name="gcn_step",
        )(adj, features, w_one, w_two.T, labels.reshape(1, BLK), mask.reshape(1, BLK))
        return loss.reshape(()), dw1, dw2.T

    row_spec = P(("nodes", "rep"))
    return jax.shard_map(local_step, mesh=mesh, in_specs=(P("nodes", None), P(("nodes", "rep"), None), P(), P(), row_spec, row_spec),
                         out_specs=(P(), P(), P()), check_vma=False)
```

```python
import functools

import jax
import jax.numpy as jnp
from jax import lax
from jax.experimental import pallas as pl
from jax.experimental.pallas import tpu as pltpu
from jax.sharding import PartitionSpec as P

BF = jnp.bfloat16
F32 = jnp.float32
BLK = 64
NEG = -1e30


def ring_order(n):
    return sorted(range(1, n), key=lambda d: (min(d, n - d), d))


def pack(v):
    out = []
    lane = lax.broadcasted_iota(jnp.int32, (BLK // 2, 128), 1)
    for k in range(v.shape[0] // BLK):
        lo, hi = v[k * BLK:(k + 1) * BLK, :128], v[k * BLK:(k + 1) * BLK, 128:]
        out += [lo, jnp.where(lane < 64, hi[:BLK // 2], pltpu.roll(hi[BLK // 2:], 64, 1))]
    return jnp.concatenate(out, axis=0)


def unpack(p):
    lane = lax.broadcasted_iota(jnp.int32, (BLK // 2, 128), 1)
    t = p[BLK:]
    hi = jnp.concatenate([jnp.where(lane < 64, t, 0.0), jnp.where(lane < 64, pltpu.roll(t, 64, 1), 0.0)], axis=0)
    return jnp.concatenate([p[:BLK], hi], axis=1)


def step_kernel(ZN, YN, XN, names, *refs):
    R = dict(zip(names, refs))
    a_hbm, x_ref, w1_ref, w2_ref = R["a"], R["x"], R["w1"], R["w2"]
    af, ac, ab, at, w2p, mt = R["af"], R["ac"], R["ab"], R["at"], R["w2p"], R["mt"]
    rep_n, node_n = ZN * YN, 2 * XN
    r, i = lax.axis_index("rep"), lax.axis_index("nodes")
    z, y = r // YN, lax.rem(r, YN)
    x, c = i // 2, lax.rem(i, 2)
    classes, hidden = w2_ref.shape
    f_in = x_ref.shape[1]
    PB = 96

    def dev(dz=0, dy=0, dx=0, dc=0):
        return {"rep": lax.rem(z + dz, ZN) * YN + lax.rem(y + dy, YN),
                "nodes": lax.rem(x + dx, XN) * 2 + lax.rem(c + dc, 2)}

    def node_dev(e):
        return {"rep": r, "nodes": lax.rem(i + e, node_n)}

    def rows(k, n):
        return pl.ds(pl.multiple_of(k * n, n), n)

    z_order, y_order, x_order = ring_order(ZN), ring_order(YN), ring_order(XN)
    peers = [dev(dz=d) for d in z_order] + [dev(dy=d) for d in y_order] + [node_dev(e) for e in range(1, node_n)]

    rows_z = YN * BLK
    n_q = node_n * ZN

    @pl.loop(0, n_q)
    def _(q):
        pltpu.make_async_copy(
            a_hbm.at[rows(z, rows_z), pl.ds(pl.multiple_of(q * (YN * BLK) + (y // 2) * 128, 128), 128)],
            af.at[:, rows(q, 128)], R["sem_af"]).start()

    @pl.loop(0, node_n)
    def _(j):
        pltpu.make_async_copy(
            a_hbm.at[:, pl.ds(pl.multiple_of(j * (rep_n * BLK) + (r // 2) * 128, 128), 128)],
            ab.at[j], R["sem_ab"]).start()

    barrier = pltpu.get_barrier_semaphore()
    for peer in peers:
        pl.semaphore_signal(barrier, inc=1, device_id=peer, device_id_type=pl.DeviceIdType.MESH)

    xg, yg, y2g, g2g, g1g = R["xg"], R["yg"], R["y2g"], R["g2g"], R["g1g"]
    own_f = (c * ZN + z) * XN + x
    xg[rows(own_f, BLK), :] = x_ref[...]
    w2p[...] = jnp.zeros_like(w2p)
    w2p[:classes, :] = w2_ref[...].astype(BF)
    b1 = w1_ref[...].astype(BF)
    mask_row = R["msk"][...].astype(F32)
    mt[0] = jnp.broadcast_to(jnp.sum(mask_row, axis=1, keepdims=True), mt.shape[1:])

    pltpu.make_async_copy(af, af, R["sem_af"]).wait()

    def select(lo):
        @pl.loop(0, n_q // 8)
        def _(step):
            for u in range(4):
                p = step * 4 + u
                xp = lax.rem(p, XN // 2)
                zk = lax.rem(p // (XN // 2), ZN)
                ck = p // (XN // 2 * ZN)
                q = (4 * xp + ck) * ZN + zk
                even, odd = af[:, rows(q, 128)], af[:, rows(q + 2 * ZN, 128)]
                ac[:, rows(p, 128)] = jnp.concatenate([even[:, lo:lo + BLK], odd[:, lo:lo + BLK]], axis=1)

    @pl.when(lax.rem(y, 2) == 0)
    def _():
        select(0)

    @pl.when(lax.rem(y, 2) == 1)
    def _():
        select(BLK)

    pl.semaphore_wait(barrier, len(peers))

    pending = []

    def send(src, dst, ssem, rsem, device):
        cp = pltpu.make_async_remote_copy(src_ref=src, dst_ref=dst, send_sem=ssem, recv_sem=rsem,
                                          device_id=device, device_id_type=pl.DeviceIdType.MESH)
        cp.start()
        pending.append(cp)
        return cp

    def gather(g, buf, index, size, n, me, peer_of, done, hooks):
        zs, zr, ss, sr = R["zs"], R["zr"], R["ss"], R["sr"]

        def slot(zk):
            return buf.at[rows(index(zk, me), size)]

        def zof(k):
            return lax.rem(z + ZN - k, ZN)

        line = {}

        def spread(k):
            mine = slot(zof(k))
            line[k] = [send(mine, mine, ss.at[g, k, e], sr.at[g, k, e], peer_of(e)) for e in ring_order(n)]

        zc = {d: send(slot(z), slot(z), zs.at[g, d], zr.at[g, d], dev(dz=d)) for d in z_order[:2]}
        spread(0)
        zc.update({d: send(slot(z), slot(z), zs.at[g, d], zr.at[g, d], dev(dz=d)) for d in z_order[2:]})
        lines = [0] + z_order
        events = []
        for s, d in enumerate(z_order):
            events.append((True, d))
            if s in (3, 5):
                events.append((False, lines.pop(0)))
        events += [(False, k) for k in lines]
        for s, (first, k) in enumerate(events):
            hooks(s)
            if first:
                zc[k].wait_recv()
                spread(k)
            else:
                for cp in line[k]:
                    cp.wait_recv()
                done(zof(k), k)

    TR = min(512, at.shape[1])

    def transpose_part(j, q):
        if j == q == 0:
            pltpu.make_async_copy(ab, ab, R["sem_ab"]).wait()
        t = ab[(j % XN) * 2 + j // XN, q * TR:(q + 1) * TR, :].T

        @pl.when(lax.rem(r, 2) == 0)
        def _():
            at[j * BLK:(j + 1) * BLK, q * TR:(q + 1) * TR] = t[:BLK]

        @pl.when(lax.rem(r, 2) == 1)
        def _():
            at[j * BLK:(j + 1) * BLK, q * TR:(q + 1) * TR] = t[BLK:]

    fillers = [functools.partial(transpose_part, j, q) for j in range(node_n) for q in range(at.shape[1] // TR)]

    def fill(n):
        for _ in range(min(n, len(fillers))):
            fillers.pop(0)()

    def fill_hook(s):
        if s < 8:
            fill(1)

    def unpack_rows(buf, first_block, n, out):
        for k in range(n):
            base = pl.multiple_of((first_block + k) * PB, 32)
            orow = pl.multiple_of((first_block + k) * BLK, BLK)
            t = buf[pl.ds(base + BLK, BLK // 2), :]
            out[pl.ds(orow, BLK), :128] = buf[pl.ds(base, BLK), :]
            out[pl.ds(orow, BLK // 2), 128:] = t
            out[pl.ds(orow + BLK // 2, BLK // 2), 128:] = jnp.concatenate([t[:, 64:], t[:, :64]], axis=1)

    zacc = R["zacc"]

    def fwd_gather(g, buf, size, prepare):
        late = []

        def line(ck, zk):
            return buf.at[rows(ck * ZN + zk, XN * size)]

        def add(ck, zk, first):
            k = ck * ZN + zk
            prepare(k)
            v = jnp.dot(ac[:, rows(k, XN * BLK)], yg[g, rows(k, XN * BLK), :], preferred_element_type=F32)
            if first:
                zacc[...] = v
            else:
                zacc[...] += v

        def partner():
            cp, zk = late.pop(0)
            cp.wait_recv()
            add(1 - c, zk, False)

        def done(zk, k):
            mine = line(c, zk)
            late.append((send(mine, mine, R["cs"].at[g, k], R["cr"].at[g, k], dev(dc=1)), zk))
            add(c, zk, k == 0)
            if len(late) > 2:
                partner()

        gather(g, buf, lambda zk, xk: (c * ZN + zk) * XN + xk, size, XN, x, lambda e: dev(dx=e), done, fill_hook)
        while late:
            partner()

    def fwd_reduce(g, packed, n_fill):
        zp, zr = (R["zpp"], R["zrp"]) if packed else (R["zp"], R["zrw"])
        v = zacc[...]
        for k in range(YN):
            piece = v[k * BLK:(k + 1) * BLK]
            zp[k] = pack(piece) if packed else piece
        cps = [send(zp.at[lax.rem(y + e, YN)], zr.at[e], R["rs"].at[g, e], R["rr"].at[g, e], dev(dy=e)) for e in y_order]
        fill(n_fill)
        total = zp[y]
        for e, cp in zip(y_order, cps):
            cp.wait_recv()
            total = total + zr[e]
        return unpack(total) if packed else total

    def exchange_small(k, src, buf, order, peer_of):
        return [send(src, buf.at[e], R["ms"].at[k, e], R["mr"].at[k, e], peer_of(e)) for e in order]

    def small_sum(k, cps, order, buf, nxt):
        s = mt[k]
        for e, cp in zip(order, cps):
            cp.wait_recv()
            s = s + buf[e]
        mt[nxt] = s

    def y1_rows(k):
        rr = rows(k, XN * BLK)
        yg[0, rr, :] = jnp.dot(xg[rr, :], b1, preferred_element_type=F32).astype(BF)

    def y2_rows(k):
        unpack_rows(y2g, k * XN, XN, yg.at[1])

    mzc = exchange_small(0, mt.at[0], R["mz"], z_order, lambda e: dev(dz=e))
    fwd_gather(0, xg, BLK, y1_rows)
    small_sum(0, mzc, z_order, R["mz"], 1)
    mxc = exchange_small(1, mt.at[1], R["mx"], x_order, lambda e: dev(dx=e))
    z1 = fwd_reduce(0, False, 10)
    R["z1s"][...] = z1
    h1 = jnp.maximum(z1, 0.0).astype(BF)
    R["h1s"][...] = h1
    nt = (((1,), (1,)), ((), ()))
    y2 = lax.dot_general(h1, w2p[...], nt, preferred_element_type=F32)
    y2g[rows(own_f, PB), :] = pack(y2).astype(BF)
    small_sum(1, mxc, x_order, R["mx"], 2)
    myc = exchange_small(2, mt.at[2], R["my"], y_order, lambda e: dev(dy=e))
    fwd_gather(1, y2g, PB, y2_rows)
    small_sum(2, myc, y_order, R["my"], 3)
    mcc = exchange_small(3, mt.at[3], R["mc"], [1], lambda e: dev(dc=e))
    z2 = fwd_reduce(1, True, 99)
    small_sum(3, mcc, [1], R["mc"], 4)

    count = mt[4][:1, :1]
    diag = lax.broadcasted_iota(jnp.int32, (BLK, BLK), 0) == lax.broadcasted_iota(jnp.int32, (BLK, BLK), 1)
    labf = jnp.sum(jnp.where(diag, jnp.broadcast_to(R["lab"][...].astype(F32), (BLK, BLK)), 0.0), axis=1, keepdims=True)
    mskf = jnp.sum(jnp.where(diag, jnp.broadcast_to(mask_row, (BLK, BLK)), 0.0), axis=1, keepdims=True)
    lane = lax.broadcasted_iota(jnp.int32, z2.shape, 1)
    logits = jnp.where(lane < classes, z2, NEG)
    shifted = logits - jnp.max(logits, axis=1, keepdims=True)
    log_probs = shifted - jnp.log(jnp.sum(jnp.exp(shifted), axis=1, keepdims=True))
    onehot = jnp.where(lane.astype(F32) == labf, 1.0, 0.0)
    g2 = (jnp.exp(log_probs) - onehot) * (mskf / count)
    g2g[rows(r, PB), :] = pack(g2).astype(BF)
    local_loss = -jnp.sum(mskf * jnp.sum(onehot * log_probs, axis=1, keepdims=True), axis=0, keepdims=True)

    dacc = R["dacc"]

    def bwd(g, buf, size, packed, hooks, late=lambda: None):
        gu = R["gu"] if packed else buf

        def done(zk, k):
            if packed:
                unpack_rows(buf, zk * YN, YN, gu)
            rr = rows(zk, YN * BLK)
            v = jnp.dot(at[:, rr], gu[rr, :], preferred_element_type=F32)
            if k == 0:
                dacc[...] = v
            else:
                dacc[...] += v

        gather(g, buf, lambda zk, yk: zk * YN + yk, size, YN, y, lambda e: dev(dy=e), done, hooks)
        dp, dr, dsum, dx = (R["dpp"], R["drp"], R["dsp"], R["dxp"]) if packed else (R["dp"], R["dr"], R["ds"], R["dx"])
        for k in range(2):
            for j in range(XN):
                piece = dacc[(k * XN + j) * BLK:(k * XN + j + 1) * BLK]
                dp[k, j] = pack(piece) if packed else piece
        cp = send(dp.at[1 - c], dr, R["cs"].at[g, 0], R["cr"].at[g, 0], dev(dc=1))
        cp.wait_recv()
        dsum[...] = dp[c] + dr[...]
        cps = [send(dsum.at[lax.rem(x + e, XN)], dx.at[e], R["rs"].at[g, e], R["rr"].at[g, e], dev(dx=e)) for e in x_order]
        late()
        total = dsum[x]
        for e, cp in zip(x_order, cps):
            cp.wait_recv()
            total = total + dx[e]
        return (unpack(total) if packed else total).astype(BF)

    def all_reduce(t, pay, payx, payy, payz, fin):
        rx = pay.shape[0] // node_n
        ry = rx // YN
        fs, fr = R["fs"], R["fr"]
        state = {}
        others = range(1, node_n)
        small = pl.ds(pl.multiple_of(i * rx + y * ry, 8), ry)

        def total(first, buf, order):
            for e, cp in zip(order, state["cp"]):
                cp.wait_recv()
                first = first + buf[e]
            return first

        def s0():
            state["cp"] = [send(pay.at[rows(lax.rem(i + e, node_n), rx)], payx.at[e], fs.at[t, 0, e], fr.at[t, 0, e], node_dev(e)) for e in others]

        def s1():
            payx[0] = total(pay[rows(i, rx)], payx, others)
            state["cp"] = [send(payx.at[0, rows(lax.rem(y + e, YN), ry)], payy.at[e], fs.at[t, 1, e], fr.at[t, 1, e], dev(dy=e)) for e in y_order]

        def s2():
            payz[z] = total(payx[0, rows(y, ry)], payy, y_order)
            state["cp"] = [send(payz.at[z], payz.at[z], fs.at[t, 2, d], fr.at[t, 2, d], dev(dz=d)) for d in z_order]

        def s3():
            for cp in state["cp"]:
                cp.wait_recv()
            s = payz[0]
            for k in range(1, ZN):
                s = s + payz[k]
            fin[small] = s
            state["cp"] = [send(fin.at[small], fin.at[small], fs.at[t, 3, e], fr.at[t, 3, e], dev(dy=e)) for e in y_order]

        def s4():
            for cp in state["cp"]:
                cp.wait_recv()
            mine = fin.at[rows(i, rx)]
            state["cp"] = [send(mine, mine, fs.at[t, 4, e], fr.at[t, 4, e], node_dev(e)) for e in others]

        def s5():
            for cp in state["cp"]:
                cp.wait_recv()

        return [s0, s1, s2, s3, s4, s5]

    d2 = bwd(2, g2g, PB, True, lambda s: None)
    tn = (((0,), (0,)), ((), ()))
    dh1 = jnp.dot(d2, w2p[...], preferred_element_type=F32)
    g1g[rows(r, BLK), :] = jnp.where(R["z1s"][...] > 0, dh1, 0.0).astype(BF)
    R["d2s"][...] = d2
    ar2 = all_reduce(0, R["pay2"], R["payx2"], R["payy2"], R["payz2"], R["fin2"])

    def make_dw2():
        dw2 = lax.dot_general(R["d2s"][...], R["h1s"][...], tn, preferred_element_type=F32)
        row = lax.broadcasted_iota(jnp.int32, (256, 128), 0)
        lane2 = lax.broadcasted_iota(jnp.int32, (256, 128), 1)
        R["pay2"][0:256] = jnp.where(jnp.logical_and(row == 255, lane2 == 127), local_loss, dw2[:, :128])
        R["pay2"][256:512] = dw2[:, 128:]
        ar2[0]()

    beside = {0: make_dw2, 8: ar2[1], 11: ar2[2]}
    n_ev = 2 * ZN - 1

    def beside_hook(s):
        for k in sorted(beside):
            if k == s or (s == n_ev - 1 and k > s):
                beside[k]()

    d1 = bwd(3, g1g, BLK, False, beside_hook, ar2[3])
    dw1 = lax.dot_general(x_ref[...], d1, tn, preferred_element_type=F32)
    R["pay1"][0:f_in] = dw1[:, :128]
    R["pay1"][f_in:2 * f_in] = dw1[:, 128:]
    ar1 = all_reduce(1, R["pay1"], R["payx1"], R["payy1"], R["payz1"], R["fin1"])
    for s in range(6):
        ar1[s]()
        if s == 1:
            ar2[4]()
    ar2[5]()
    fin1, fin2 = R["fin1"], R["fin2"]
    R["dw2"][:, :128] = fin2[0:classes]
    R["dw2"][:, 128:] = fin2[256:256 + classes]
    R["loss"][0, 0] = jnp.sum(fin2[255:256, 127:] / count)
    R["dw1"][:, :128] = fin1[0:f_in]
    R["dw1"][:, 128:] = fin1[f_in:2 * f_in]
    for cp in pending:
        cp.wait_send()


def solution(mesh):
    rep_n, node_n = mesh.shape["rep"], mesh.shape["nodes"]
    YN = 4
    ZN = rep_n // YN
    XN = node_n // 2

    def local_step(adj, features, w_one, w_two, labels, mask):
        f_in, hidden = w_one.shape
        classes = w_two.shape[1]
        rows_g = adj.shape[0]
        blocks_y = node_n * ZN
        V = pltpu.VMEM
        D = pltpu.SemaphoreType.DMA

        def reduce_bufs(t, n):
            rx = n // node_n
            return {f"pay{t}": V((n, 128), F32), f"payx{t}": V((node_n, rx, 128), F32),
                    f"payy{t}": V((YN, rx // YN, 128), F32), f"payz{t}": V((ZN, rx // YN, 128), F32), f"fin{t}": V((n, 128), F32)}

        scratch = dict(
            af=V((YN * BLK, blocks_y * 128), BF), ac=V((YN * BLK, blocks_y * BLK), BF),
            ab=V((node_n, rows_g, 128), BF), at=V((node_n * BLK, rows_g), BF),
            xg=V((blocks_y * BLK, f_in), BF), yg=V((2, blocks_y * BLK, 256), BF), y2g=V((blocks_y * 96, 128), BF),
            g2g=V((rep_n * 96, 128), BF), gu=V((rows_g, 256), BF), g1g=V((rows_g, hidden), BF),
            zacc=V((YN * BLK, 256), F32), dacc=V((node_n * BLK, 256), F32),
            zp=V((YN, BLK, 256), F32), zrw=V((YN, BLK, 256), F32), zpp=V((YN, 96, 128), F32), zrp=V((YN, 96, 128), F32),
            dp=V((2, XN, BLK, 256), F32), dr=V((XN, BLK, 256), F32), ds=V((XN, BLK, 256), F32), dx=V((XN, BLK, 256), F32),
            dpp=V((2, XN, 96, 128), F32), drp=V((XN, 96, 128), F32), dsp=V((XN, 96, 128), F32), dxp=V((XN, 96, 128), F32),
            mt=V((5, 8, 128), F32), mz=V((ZN, 8, 128), F32), mx=V((XN, 8, 128), F32), my=V((YN, 8, 128), F32),
            mc=V((2, 8, 128), F32),
            z1s=V((BLK, hidden), F32), h1s=V((BLK, hidden), BF), d2s=V((BLK, 256), BF), w2p=V((256, hidden), BF),
            sem_af=D, sem_ab=D,
            zs=D((4, 8)), zr=D((4, 8)), ss=D((4, 8, 4)), sr=D((4, 8, 4)), cs=D((4, 8)), cr=D((4, 8)),
            rs=D((4, 4)), rr=D((4, 4)), ms=D((4, 8)), mr=D((4, 8)), fs=D((2, 7, 8)), fr=D((2, 7, 8)),
        )
        scratch.update(reduce_bufs(1, 2 * f_in))
        scratch.update(reduce_bufs(2, 512))
        names = ["a", "x", "w1", "w2", "lab", "msk", "loss", "dw1", "dw2"] + list(scratch)
        vm = pl.BlockSpec(memory_space=pltpu.VMEM)
        loss, dw1, dw2 = pl.pallas_call(
            functools.partial(step_kernel, ZN, YN, XN, names),
            out_shape=(jax.ShapeDtypeStruct((1, 1), F32), jax.ShapeDtypeStruct((f_in, hidden), F32),
                       jax.ShapeDtypeStruct((classes, hidden), F32)),
            in_specs=[pl.BlockSpec(memory_space=pl.ANY), vm, vm, vm, vm, vm],
            out_specs=(pl.BlockSpec(memory_space=pltpu.SMEM), vm, vm),
            scratch_shapes=list(scratch.values()),
            compiler_params=pltpu.CompilerParams(collective_id=0, has_side_effects=True, vmem_limit_bytes=60 * 2 ** 20),
            name="gcn_step",
        )(adj, features, w_one, w_two.T, labels.reshape(1, BLK), mask.reshape(1, BLK))
        return loss.reshape(()), dw1, dw2.T

    row_spec = P(("nodes", "rep"))
    return jax.shard_map(local_step, mesh=mesh, in_specs=(P("nodes", None), P(("nodes", "rep"), None), P(), P(), row_spec, row_spec),
                         out_specs=(P(), P(), P()), check_vma=False)
```

```python
import functools

import jax
import jax.numpy as jnp
from jax import lax
from jax.experimental import pallas as pl
from jax.experimental.pallas import tpu as pltpu
from jax.sharding import PartitionSpec as P

BF = jnp.bfloat16
F32 = jnp.float32
BLK = 64
NEG = -1e30


def ring_order(n):
    return sorted(range(1, n), key=lambda d: (min(d, n - d), d))


def pack(v):
    out = []
    lane = lax.broadcasted_iota(jnp.int32, (BLK // 2, 128), 1)
    for k in range(v.shape[0] // BLK):
        lo, hi = v[k * BLK:(k + 1) * BLK, :128], v[k * BLK:(k + 1) * BLK, 128:]
        out += [lo, jnp.where(lane < 64, hi[:BLK // 2], pltpu.roll(hi[BLK // 2:], 64, 1))]
    return jnp.concatenate(out, axis=0)


def unpack(p):
    lane = lax.broadcasted_iota(jnp.int32, (BLK // 2, 128), 1)
    t = p[BLK:]
    hi = jnp.concatenate([jnp.where(lane < 64, t, 0.0), jnp.where(lane < 64, pltpu.roll(t, 64, 1), 0.0)], axis=0)
    return jnp.concatenate([p[:BLK], hi], axis=1)


def step_kernel(ZN, YN, XN, names, *refs):
    R = dict(zip(names, refs))
    a_hbm, x_ref, w1_ref, w2_ref = R["a"], R["x"], R["w1"], R["w2"]
    af, ac, ab, at, w2p, mt = R["af"], R["ac"], R["ab"], R["at"], R["w2p"], R["mt"]
    rep_n, node_n = ZN * YN, 2 * XN
    r, i = lax.axis_index("rep"), lax.axis_index("nodes")
    z, y = r // YN, lax.rem(r, YN)
    x, c = i // 2, lax.rem(i, 2)
    classes, hidden = w2_ref.shape
    f_in = x_ref.shape[1]
    PB = 96

    def dev(dz=0, dy=0, dx=0, dc=0):
        return {"rep": lax.rem(z + dz, ZN) * YN + lax.rem(y + dy, YN),
                "nodes": lax.rem(x + dx, XN) * 2 + lax.rem(c + dc, 2)}

    def node_dev(e):
        return {"rep": r, "nodes": lax.rem(i + e, node_n)}

    def rows(k, n):
        return pl.ds(pl.multiple_of(k * n, n), n)

    z_order, y_order, x_order = ring_order(ZN), ring_order(YN), ring_order(XN)
    peers = [dev(dz=d) for d in z_order] + [dev(dy=d) for d in y_order] + [node_dev(e) for e in range(1, node_n)]

    rows_z = YN * BLK
    n_q = node_n * ZN

    @pl.loop(0, n_q)
    def _(q):
        pltpu.make_async_copy(
            a_hbm.at[rows(z, rows_z), pl.ds(pl.multiple_of(q * (YN * BLK) + (y // 2) * 128, 128), 128)],
            af.at[:, rows(q, 128)], R["sem_af"]).start()

    barrier = pltpu.get_barrier_semaphore()
    for peer in peers:
        pl.semaphore_signal(barrier, inc=1, device_id=peer, device_id_type=pl.DeviceIdType.MESH)

    xg, yg, y2g, g2g, g1g = R["xg"], R["yg"], R["y2g"], R["g2g"], R["g1g"]
    own_f = (c * ZN + z) * XN + x
    xg[rows(own_f, BLK), :] = x_ref[...]
    w2p[...] = jnp.zeros_like(w2p)
    w2p[:classes, :] = w2_ref[...].astype(BF)
    b1 = w1_ref[...].astype(BF)
    mask_row = R["msk"][...].astype(F32)
    mt[0] = jnp.broadcast_to(jnp.sum(mask_row, axis=1, keepdims=True), mt.shape[1:])

    pl.semaphore_wait(barrier, len(peers))

    pending = []

    def drain(keep):
        while len(pending) > keep:
            pending.pop(0).wait_send()

    def send(src, dst, ssem, rsem, device):
        cp = pltpu.make_async_remote_copy(src_ref=src, dst_ref=dst, send_sem=ssem, recv_sem=rsem,
                                          device_id=device, device_id_type=pl.DeviceIdType.MESH)
        cp.start()
        pending.append(cp)
        return cp

    def gather(g, buf, index, size, n, me, peer_of, done, hooks, z_ahead=False):
        zs, zr, ss, sr = R["zs"], R["zr"], R["ss"], R["sr"]

        def slot(zk):
            return buf.at[rows(index(zk, me), size)]

        def zof(k):
            return lax.rem(z + ZN - k, ZN)

        line = {}

        def spread(k):
            mine = slot(zof(k))
            line[k] = [send(mine, mine, ss.at[g, k, e], sr.at[g, k, e], peer_of(e)) for e in ring_order(n)]

        zc = {d: send(slot(z), slot(z), zs.at[g, d], zr.at[g, d], dev(dz=d)) for d in z_order[:2]}
        spread(0)
        zc.update({d: send(slot(z), slot(z), zs.at[g, d], zr.at[g, d], dev(dz=d)) for d in z_order[2:]})
        lines = [0] + z_order
        events = []
        for s, d in enumerate(z_order):
            events.append((True, d))
            if s in (3, 5) and not z_ahead:
                events.append((False, lines.pop(0)))
        events += [(False, k) for k in lines]
        for s, (first, k) in enumerate(events):
            hooks(s)
            if first:
                zc[k].wait_recv()
                spread(k)
            else:
                for cp in line[k]:
                    cp.wait_recv()
                done(zof(k), k)

    def select(p, lo):
        xp, zk, ck = p % (XN // 2), p // (XN // 2) % ZN, p // (XN // 2 * ZN)
        q = (4 * xp + ck) * ZN + zk
        even, odd = af[:, q * 128:(q + 1) * 128], af[:, (q + 2 * ZN) * 128:(q + 2 * ZN + 1) * 128]
        ac[:, p * 128:(p + 1) * 128] = jnp.concatenate([even[:, lo:lo + BLK], odd[:, lo:lo + BLK]], axis=1)

    n_sel = n_q // 2

    def select_hook(s):
        if s == 0:
            pltpu.make_async_copy(af, af, R["sem_af"]).wait()
            start_ab()
        steps = ZN - 1
        if s >= steps:
            return
        todo = range(s * n_sel // steps, (s + 1) * n_sel // steps)

        @pl.when(lax.rem(y, 2) == 0)
        def _():
            for p in todo:
                select(p, 0)

        @pl.when(lax.rem(y, 2) == 1)
        def _():
            for p in todo:
                select(p, BLK)

    def start_ab():
        @pl.loop(0, node_n)
        def _(j):
            pltpu.make_async_copy(
                a_hbm.at[:, pl.ds(pl.multiple_of(j * (rep_n * BLK) + (r // 2) * 128, 128), 128)],
                ab.at[j], R["sem_ab"]).start()

    TR = min(512, at.shape[1])

    def transpose_part(j, q):
        if j == q == 0:
            pltpu.make_async_copy(ab, ab, R["sem_ab"]).wait()
        t = ab[(j % XN) * 2 + j // XN, q * TR:(q + 1) * TR, :].T

        @pl.when(lax.rem(r, 2) == 0)
        def _():
            at[j * BLK:(j + 1) * BLK, q * TR:(q + 1) * TR] = t[:BLK]

        @pl.when(lax.rem(r, 2) == 1)
        def _():
            at[j * BLK:(j + 1) * BLK, q * TR:(q + 1) * TR] = t[BLK:]

    fillers = [functools.partial(transpose_part, j, q) for j in range(node_n) for q in range(at.shape[1] // TR)]

    def fill(n):
        for _ in range(min(n, len(fillers))):
            fillers.pop(0)()

    def fill_hook(s):
        if s < 8:
            fill(1)

    def unpack_rows(buf, first_block, n, out):
        for k in range(n):
            base = pl.multiple_of((first_block + k) * PB, 32)
            orow = pl.multiple_of((first_block + k) * BLK, BLK)
            t = buf[pl.ds(base + BLK, BLK // 2), :]
            out[pl.ds(orow, BLK), :128] = buf[pl.ds(base, BLK), :]
            out[pl.ds(orow, BLK // 2), 128:] = t
            out[pl.ds(orow + BLK // 2, BLK // 2), 128:] = jnp.concatenate([t[:, 64:], t[:, :64]], axis=1)

    zacc = R["zacc"]

    def fwd_gather(g, buf, size, prepare, hooks, z_ahead):
        late = []

        def line(ck, zk):
            return buf.at[rows(ck * ZN + zk, XN * size)]

        def add(ck, zk, first):
            k = ck * ZN + zk
            prepare(k)
            v = jnp.dot(ac[:, rows(k, XN * BLK)], yg[g, rows(k, XN * BLK), :], preferred_element_type=F32)
            if first:
                zacc[...] = v
            else:
                zacc[...] += v

        def partner():
            cp, zk = late.pop(0)
            cp.wait_recv()
            add(1 - c, zk, False)

        def done(zk, k):
            mine = line(c, zk)
            late.append((send(mine, mine, R["cs"].at[g, k], R["cr"].at[g, k], dev(dc=1)), zk))
            add(c, zk, k == 0)
            if len(late) > 2:
                partner()

        gather(g, buf, lambda zk, xk: (c * ZN + zk) * XN + xk, size, XN, x, lambda e: dev(dx=e), done, hooks, z_ahead)
        while late:
            partner()

    def fwd_reduce(g, packed, n_fill):
        zp, zr = (R["zpp"], R["zrp"]) if packed else (R["zp"], R["zrw"])
        v = zacc[...]
        for k in range(YN):
            piece = v[k * BLK:(k + 1) * BLK]
            zp[k] = pack(piece) if packed else piece
        cps = [send(zp.at[lax.rem(y + e, YN)], zr.at[e], R["rs"].at[g, e], R["rr"].at[g, e], dev(dy=e)) for e in y_order]
        fill(n_fill)
        drain(len(cps))
        total = zp[y]
        for e, cp in zip(y_order, cps):
            cp.wait_recv()
            total = total + zr[e]
        return unpack(total) if packed else total

    def exchange_small(k, src, buf, order, peer_of):
        return [send(src, buf.at[e], R["ms"].at[k, e], R["mr"].at[k, e], peer_of(e)) for e in order]

    def small_sum(k, cps, order, buf, nxt):
        s = mt[k]
        for e, cp in zip(order, cps):
            cp.wait_recv()
            s = s + buf[e]
        mt[nxt] = s

    def y1_rows(k):
        rr = rows(k, XN * BLK)
        yg[0, rr, :] = jnp.dot(xg[rr, :], b1, preferred_element_type=F32).astype(BF)

    def y2_rows(k):
        unpack_rows(y2g, k * XN, XN, yg.at[1])

    mzc = exchange_small(0, mt.at[0], R["mz"], z_order, lambda e: dev(dz=e))
    fwd_gather(0, xg, BLK, y1_rows, select_hook, True)
    small_sum(0, mzc, z_order, R["mz"], 1)
    mxc = exchange_small(1, mt.at[1], R["mx"], x_order, lambda e: dev(dx=e))
    z1 = fwd_reduce(0, False, 14)
    R["z1s"][...] = z1
    h1 = jnp.maximum(z1, 0.0).astype(BF)
    R["h1s"][...] = h1
    nt = (((1,), (1,)), ((), ()))
    y2 = lax.dot_general(h1, w2p[...], nt, preferred_element_type=F32)
    y2g[rows(own_f, PB), :] = pack(y2).astype(BF)
    small_sum(1, mxc, x_order, R["mx"], 2)
    myc = exchange_small(2, mt.at[2], R["my"], y_order, lambda e: dev(dy=e))
    fwd_gather(1, y2g, PB, y2_rows, fill_hook, False)
    small_sum(2, myc, y_order, R["my"], 3)
    mcc = exchange_small(3, mt.at[3], R["mc"], [1], lambda e: dev(dc=e))
    z2 = fwd_reduce(1, True, 99)
    small_sum(3, mcc, [1], R["mc"], 4)

    count = mt[4][:1, :1]
    diag = lax.broadcasted_iota(jnp.int32, (BLK, BLK), 0) == lax.broadcasted_iota(jnp.int32, (BLK, BLK), 1)
    labf = jnp.sum(jnp.where(diag, jnp.broadcast_to(R["lab"][...].astype(F32), (BLK, BLK)), 0.0), axis=1, keepdims=True)
    mskf = jnp.sum(jnp.where(diag, jnp.broadcast_to(mask_row, (BLK, BLK)), 0.0), axis=1, keepdims=True)
    lane = lax.broadcasted_iota(jnp.int32, z2.shape, 1)
    logits = jnp.where(lane < classes, z2, NEG)
    shifted = logits - jnp.max(logits, axis=1, keepdims=True)
    log_probs = shifted - jnp.log(jnp.sum(jnp.exp(shifted), axis=1, keepdims=True))
    onehot = jnp.where(lane.astype(F32) == labf, 1.0, 0.0)
    g2 = (jnp.exp(log_probs) - onehot) * (mskf / count)
    g2g[rows(r, PB), :] = pack(g2).astype(BF)
    local_loss = -jnp.sum(mskf * jnp.sum(onehot * log_probs, axis=1, keepdims=True), axis=0, keepdims=True)

    dacc = R["dacc"]

    def bwd(g, buf, size, packed, hooks, late=lambda: None):
        gu = R["gu"] if packed else buf

        def done(zk, k):
            if packed:
                unpack_rows(buf, zk * YN, YN, gu)
            rr = rows(zk, YN * BLK)
            v = jnp.dot(at[:, rr], gu[rr, :], preferred_element_type=F32)
            if k == 0:
                dacc[...] = v
            else:
                dacc[...] += v

        gather(g, buf, lambda zk, yk: zk * YN + yk, size, YN, y, lambda e: dev(dy=e), done, hooks)
        dp, dr, dsum, dx = (R["dpp"], R["drp"], R["dsp"], R["dxp"]) if packed else (R["dp"], R["dr"], R["ds"], R["dx"])
        for k in range(2):
            for j in range(XN):
                piece = dacc[(k * XN + j) * BLK:(k * XN + j + 1) * BLK]
                dp[k, j] = pack(piece) if packed else piece
        cp = send(dp.at[1 - c], dr, R["cs"].at[g, 0], R["cr"].at[g, 0], dev(dc=1))
        cp.wait_recv()
        dsum[...] = dp[c] + dr[...]
        cps = [send(dsum.at[lax.rem(x + e, XN)], dx.at[e], R["rs"].at[g, e], R["rr"].at[g, e], dev(dx=e)) for e in x_order]
        late()
        drain(len(cps) + 3)
        total = dsum[x]
        for e, cp in zip(x_order, cps):
            cp.wait_recv()
            total = total + dx[e]
        return (unpack(total) if packed else total).astype(BF)

    def all_reduce(t, pay, payx, payy, payz, fin):
        rx = pay.shape[0] // node_n
        ry = rx // YN
        fs, fr = R["fs"], R["fr"]
        state = {}
        others = range(1, node_n)
        small = pl.ds(pl.multiple_of(i * rx + y * ry, 8), ry)

        def total(first, buf, order):
            for e, cp in zip(order, state["cp"]):
                cp.wait_recv()
                first = first + buf[e]
            return first

        def s0():
            state["cp"] = [send(pay.at[rows(lax.rem(i + e, node_n), rx)], payx.at[e], fs.at[t, 0, e], fr.at[t, 0, e], node_dev(e)) for e in others]

        def s1():
            payx[0] = total(pay[rows(i, rx)], payx, others)
            state["cp"] = [send(payx.at[0, rows(lax.rem(y + e, YN), ry)], payy.at[e], fs.at[t, 1, e], fr.at[t, 1, e], dev(dy=e)) for e in y_order]

        def s2():
            payz[z] = total(payx[0, rows(y, ry)], payy, y_order)
            state["cp"] = [send(payz.at[z], payz.at[z], fs.at[t, 2, d], fr.at[t, 2, d], dev(dz=d)) for d in z_order]

        def s3():
            for cp in state["cp"]:
                cp.wait_recv()
            s = payz[0]
            for k in range(1, ZN):
                s = s + payz[k]
            fin[small] = s
            state["cp"] = [send(fin.at[small], fin.at[small], fs.at[t, 3, e], fr.at[t, 3, e], dev(dy=e)) for e in y_order]

        def s4():
            for cp in state["cp"]:
                cp.wait_recv()
            mine = fin.at[rows(i, rx)]
            state["cp"] = [send(mine, mine, fs.at[t, 4, e], fr.at[t, 4, e], node_dev(e)) for e in others]

        def s5():
            for cp in state["cp"]:
                cp.wait_recv()

        return [s0, s1, s2, s3, s4, s5]

    d2 = bwd(2, g2g, PB, True, lambda s: None)
    tn = (((0,), (0,)), ((), ()))
    dh1 = jnp.dot(d2, w2p[...], preferred_element_type=F32)
    g1g[rows(r, BLK), :] = jnp.where(R["z1s"][...] > 0, dh1, 0.0).astype(BF)
    R["d2s"][...] = d2
    ar2 = all_reduce(0, R["pay2"], R["payx2"], R["payy2"], R["payz2"], R["fin2"])

    def make_dw2():
        dw2 = lax.dot_general(R["d2s"][...], R["h1s"][...], tn, preferred_element_type=F32)
        row = lax.broadcasted_iota(jnp.int32, (256, 128), 0)
        lane2 = lax.broadcasted_iota(jnp.int32, (256, 128), 1)
        R["pay2"][0:256] = jnp.where(jnp.logical_and(row == 255, lane2 == 127), local_loss, dw2[:, :128])
        R["pay2"][256:512] = dw2[:, 128:]
        ar2[0]()

    def beside_hook(s):
        if s == 0:
            make_dw2()

    d1 = bwd(3, g1g, BLK, False, beside_hook, ar2[1])
    dw1 = lax.dot_general(x_ref[...], d1, tn, preferred_element_type=F32)
    R["pay1"][0:f_in] = dw1[:, :128]
    R["pay1"][f_in:2 * f_in] = dw1[:, 128:]
    ar1 = all_reduce(1, R["pay1"], R["payx1"], R["payy1"], R["payz1"], R["fin1"])
    for s in range(6):
        ar1[s]()
        if s < 4:
            ar2[2 + s]()
    fin1, fin2 = R["fin1"], R["fin2"]
    R["dw2"][:, :128] = fin2[0:classes]
    R["dw2"][:, 128:] = fin2[256:256 + classes]
    R["loss"][0, 0] = jnp.sum(fin2[255:256, 127:] / count)
    R["dw1"][:, :128] = fin1[0:f_in]
    R["dw1"][:, 128:] = fin1[f_in:2 * f_in]
    for cp in pending:
        cp.wait_send()


def solution(mesh):
    rep_n, node_n = mesh.shape["rep"], mesh.shape["nodes"]
    YN = 4
    ZN = rep_n // YN
    XN = node_n // 2

    def local_step(adj, features, w_one, w_two, labels, mask):
        f_in, hidden = w_one.shape
        classes = w_two.shape[1]
        rows_g = adj.shape[0]
        blocks_y = node_n * ZN
        V = pltpu.VMEM
        D = pltpu.SemaphoreType.DMA

        def reduce_bufs(t, n):
            rx = n // node_n
            return {f"pay{t}": V((n, 128), F32), f"payx{t}": V((node_n, rx, 128), F32),
                    f"payy{t}": V((YN, rx // YN, 128), F32), f"payz{t}": V((ZN, rx // YN, 128), F32), f"fin{t}": V((n, 128), F32)}

        scratch = dict(
            af=V((YN * BLK, blocks_y * 128), BF), ac=V((YN * BLK, blocks_y * BLK), BF),
            ab=V((node_n, rows_g, 128), BF), at=V((node_n * BLK, rows_g), BF),
            xg=V((blocks_y * BLK, f_in), BF), yg=V((2, blocks_y * BLK, 256), BF), y2g=V((blocks_y * 96, 128), BF),
            g2g=V((rep_n * 96, 128), BF), gu=V((rows_g, 256), BF), g1g=V((rows_g, hidden), BF),
            zacc=V((YN * BLK, 256), F32), dacc=V((node_n * BLK, 256), F32),
            zp=V((YN, BLK, 256), F32), zrw=V((YN, BLK, 256), F32), zpp=V((YN, 96, 128), F32), zrp=V((YN, 96, 128), F32),
            dp=V((2, XN, BLK, 256), F32), dr=V((XN, BLK, 256), F32), ds=V((XN, BLK, 256), F32), dx=V((XN, BLK, 256), F32),
            dpp=V((2, XN, 96, 128), F32), drp=V((XN, 96, 128), F32), dsp=V((XN, 96, 128), F32), dxp=V((XN, 96, 128), F32),
            mt=V((5, 8, 128), F32), mz=V((ZN, 8, 128), F32), mx=V((XN, 8, 128), F32), my=V((YN, 8, 128), F32),
            mc=V((2, 8, 128), F32),
            z1s=V((BLK, hidden), F32), h1s=V((BLK, hidden), BF), d2s=V((BLK, 256), BF), w2p=V((256, hidden), BF),
            sem_af=D, sem_ab=D,
            zs=D((4, 8)), zr=D((4, 8)), ss=D((4, 8, 4)), sr=D((4, 8, 4)), cs=D((4, 8)), cr=D((4, 8)),
            rs=D((4, 4)), rr=D((4, 4)), ms=D((4, 8)), mr=D((4, 8)), fs=D((2, 7, 8)), fr=D((2, 7, 8)),
        )
        scratch.update(reduce_bufs(1, 2 * f_in))
        scratch.update(reduce_bufs(2, 512))
        names = ["a", "x", "w1", "w2", "lab", "msk", "loss", "dw1", "dw2"] + list(scratch)
        vm = pl.BlockSpec(memory_space=pltpu.VMEM)
        loss, dw1, dw2 = pl.pallas_call(
            functools.partial(step_kernel, ZN, YN, XN, names),
            out_shape=(jax.ShapeDtypeStruct((1, 1), F32), jax.ShapeDtypeStruct((f_in, hidden), F32),
                       jax.ShapeDtypeStruct((classes, hidden), F32)),
            in_specs=[pl.BlockSpec(memory_space=pl.ANY), vm, vm, vm, vm, vm],
            out_specs=(pl.BlockSpec(memory_space=pltpu.SMEM), vm, vm),
            scratch_shapes=list(scratch.values()),
            compiler_params=pltpu.CompilerParams(collective_id=0, has_side_effects=True, vmem_limit_bytes=60 * 2 ** 20),
            name="gcn_step",
        )(adj, features, w_one, w_two.T, labels.reshape(1, BLK), mask.reshape(1, BLK))
        return loss.reshape(()), dw1, dw2.T

    row_spec = P(("nodes", "rep"))
    return jax.shard_map(local_step, mesh=mesh, in_specs=(P("nodes", None), P(("nodes", "rep"), None), P(), P(), row_spec, row_spec),
                         out_specs=(P(), P(), P()), check_vma=False)
```

```python
import functools

import jax
import jax.numpy as jnp
from jax import lax
from jax.experimental import pallas as pl
from jax.experimental.pallas import tpu as pltpu
from jax.sharding import PartitionSpec as P

BF = jnp.bfloat16
F32 = jnp.float32
BLK = 64
NEG = -1e30


def ring_order(n):
    return sorted(range(1, n), key=lambda d: (min(d, n - d), d))


def pack(v):
    out = []
    lane = lax.broadcasted_iota(jnp.int32, (BLK // 2, 128), 1)
    for k in range(v.shape[0] // BLK):
        lo, hi = v[k * BLK:(k + 1) * BLK, :128], v[k * BLK:(k + 1) * BLK, 128:]
        out += [lo, jnp.where(lane < 64, hi[:BLK // 2], pltpu.roll(hi[BLK // 2:], 64, 1))]
    return jnp.concatenate(out, axis=0)


def unpack(p):
    lane = lax.broadcasted_iota(jnp.int32, (BLK // 2, 128), 1)
    t = p[BLK:]
    hi = jnp.concatenate([jnp.where(lane < 64, t, 0.0), jnp.where(lane < 64, pltpu.roll(t, 64, 1), 0.0)], axis=0)
    return jnp.concatenate([p[:BLK], hi], axis=1)


def step_kernel(ZN, YN, XN, names, *refs):
    R = dict(zip(names, refs))
    a_hbm, x_ref, w1_ref, w2_ref = R["a"], R["x"], R["w1"], R["w2"]
    af, ab, at, w2p, mt = R["af"], R["ab"], R["at"], R["w2p"], R["mt"]
    rep_n, node_n = ZN * YN, 2 * XN
    r, i = lax.axis_index("rep"), lax.axis_index("nodes")
    z, y = r // YN, lax.rem(r, YN)
    x, c = i // 2, lax.rem(i, 2)
    classes, hidden = w2_ref.shape
    f_in = x_ref.shape[1]
    PB = 96

    def dev(dz=0, dy=0, dx=0, dc=0):
        return {"rep": lax.rem(z + dz, ZN) * YN + lax.rem(y + dy, YN),
                "nodes": lax.rem(x + dx, XN) * 2 + lax.rem(c + dc, 2)}

    def node_dev(e):
        return {"rep": r, "nodes": lax.rem(i + e, node_n)}

    def rows(k, n):
        return pl.ds(pl.multiple_of(k * n, n), n)

    z_order, y_order, x_order = ring_order(ZN), ring_order(YN), ring_order(XN)
    peers = [dev(dz=d) for d in z_order] + [dev(dy=d) for d in y_order] + [node_dev(e) for e in range(1, node_n)]

    rows_z = YN * BLK
    n_q = node_n * ZN

    @pl.loop(0, n_q)
    def _(q):
        pltpu.make_async_copy(
            a_hbm.at[rows(z, rows_z), pl.ds(pl.multiple_of(q * (YN * BLK) + (y // 2) * 128, 128), 128)],
            af.at[:, rows((lax.rem(q // ZN, 2) * ZN + lax.rem(q, ZN)) * XN + q // (2 * ZN), 128)], R["sem_af"]).start()

    barrier = pltpu.get_barrier_semaphore()
    for peer in peers:
        pl.semaphore_signal(barrier, inc=1, device_id=peer, device_id_type=pl.DeviceIdType.MESH)

    xg, yg, y2g, g2g, g1g = R["xg"], R["yg"], R["y2g"], R["g2g"], R["g1g"]
    own_f = (c * ZN + z) * XN + x
    xg[rows(own_f, BLK), :] = x_ref[...]
    mine_at = lax.rem(y, 2) * BLK

    @pl.loop(0, yg.shape[1] // 128)
    def _(k):
        zero_rows = pl.ds(pl.multiple_of(k * 128 + BLK - mine_at, BLK), BLK)
        for t in range(2):
            yg[t, zero_rows, :] = jnp.zeros((BLK, 256), BF)

    w2p[...] = jnp.zeros_like(w2p)
    w2p[:classes, :] = w2_ref[...].astype(BF)
    b1 = w1_ref[...].astype(BF)
    mask_row = R["msk"][...].astype(F32)
    mt[0] = jnp.broadcast_to(jnp.sum(mask_row, axis=1, keepdims=True), mt.shape[1:])

    pl.semaphore_wait(barrier, len(peers))

    pending = []

    def drain(keep):
        while len(pending) > keep:
            pending.pop(0).wait_send()

    def send(src, dst, ssem, rsem, device):
        cp = pltpu.make_async_remote_copy(src_ref=src, dst_ref=dst, send_sem=ssem, recv_sem=rsem,
                                          device_id=device, device_id_type=pl.DeviceIdType.MESH)
        cp.start()
        pending.append(cp)
        return cp

    def gather(g, buf, index, size, n, me, peer_of, done, hooks, z_ahead=False):
        zs, zr, ss, sr = R["zs"], R["zr"], R["ss"], R["sr"]

        def slot(zk):
            return buf.at[rows(index(zk, me), size)]

        def zof(k):
            return lax.rem(z + ZN - k, ZN)

        line = {}

        def spread(k):
            mine = slot(zof(k))
            line[k] = [send(mine, mine, ss.at[g, k, e], sr.at[g, k, e], peer_of(e)) for e in ring_order(n)]

        zc = {d: send(slot(z), slot(z), zs.at[g, d], zr.at[g, d], dev(dz=d)) for d in z_order[:2]}
        spread(0)
        zc.update({d: send(slot(z), slot(z), zs.at[g, d], zr.at[g, d], dev(dz=d)) for d in z_order[2:]})
        lines = [0] + z_order
        events = []
        for s, d in enumerate(z_order):
            events.append((True, d))
            if s in (3, 5) and not z_ahead:
                events.append((False, lines.pop(0)))
        events += [(False, k) for k in lines]
        for s, (first, k) in enumerate(events):
            hooks(s)
            if first:
                zc[k].wait_recv()
                spread(k)
            else:
                for cp in line[k]:
                    cp.wait_recv()
                done(zof(k), k)

    def start_ab():
        @pl.loop(0, node_n)
        def _(j):
            pltpu.make_async_copy(
                a_hbm.at[:, pl.ds(pl.multiple_of(j * (rep_n * BLK) + (r // 2) * 128, 128), 128)],
                ab.at[j], R["sem_ab"]).start()

    TR = min(512, at.shape[1])

    def transpose_part(j, q):
        if j == q == 0:
            pltpu.make_async_copy(ab, ab, R["sem_ab"]).wait()
        t = ab[(j % XN) * 2 + j // XN, q * TR:(q + 1) * TR, :].T

        @pl.when(lax.rem(r, 2) == 0)
        def _():
            at[j * BLK:(j + 1) * BLK, q * TR:(q + 1) * TR] = t[:BLK]

        @pl.when(lax.rem(r, 2) == 1)
        def _():
            at[j * BLK:(j + 1) * BLK, q * TR:(q + 1) * TR] = t[BLK:]

    fillers = [functools.partial(transpose_part, j, q) for j in range(node_n) for q in range(at.shape[1] // TR)]

    def fill(n):
        for _ in range(min(n, len(fillers))):
            fillers.pop(0)()

    def fill_hook(s):
        if s < 8:
            fill(1)

    def unpack_rows(buf, first_block, n, out, pitch=BLK, shift=0):
        for k in range(n):
            base = pl.multiple_of((first_block + k) * PB, 32)
            orow = pl.multiple_of((first_block + k) * pitch + shift, BLK)
            t = buf[pl.ds(base + BLK, BLK // 2), :]
            out[pl.ds(orow, BLK), :128] = buf[pl.ds(base, BLK), :]
            out[pl.ds(orow, BLK // 2), 128:] = t
            out[pl.ds(orow + BLK // 2, BLK // 2), 128:] = jnp.concatenate([t[:, 64:], t[:, :64]], axis=1)

    zacc = R["zacc"]

    def fwd_gather(g, buf, size, prepare, hooks, z_ahead):
        late = []

        def line(ck, zk):
            return buf.at[rows(ck * ZN + zk, XN * size)]

        def add(ck, zk, first):
            k = ck * ZN + zk
            if first and g == 0:
                pltpu.make_async_copy(af, af, R["sem_af"]).wait()
                start_ab()
            prepare(k)
            v = jnp.dot(af[:, rows(k, XN * 128)], yg[g, rows(k, XN * 128), :], preferred_element_type=F32)
            if first:
                zacc[...] = v
            else:
                zacc[...] += v

        def partner():
            cp, zk = late.pop(0)
            cp.wait_recv()
            add(1 - c, zk, False)

        def done(zk, k):
            mine = line(c, zk)
            late.append((send(mine, mine, R["cs"].at[g, k], R["cr"].at[g, k], dev(dc=1)), zk))
            add(c, zk, k == 0)
            if len(late) > 2:
                partner()

        gather(g, buf, lambda zk, xk: (c * ZN + zk) * XN + xk, size, XN, x, lambda e: dev(dx=e), done, hooks, z_ahead)
        while late:
            partner()

    def fwd_reduce(g, packed, n_fill):
        zp, zr = (R["zpp"], R["zrp"]) if packed else (R["zp"], R["zrw"])
        v = zacc[...]
        for k in range(YN):
            piece = v[k * BLK:(k + 1) * BLK]
            zp[k] = pack(piece) if packed else piece
        cps = [send(zp.at[lax.rem(y + e, YN)], zr.at[e], R["rs"].at[g, e], R["rr"].at[g, e], dev(dy=e)) for e in y_order]
        fill(n_fill)
        drain(len(cps))
        total = zp[y]
        for e, cp in zip(y_order, cps):
            cp.wait_recv()
            total = total + zr[e]
        return unpack(total) if packed else total

    def exchange_small(k, src, buf, order, peer_of):
        return [send(src, buf.at[e], R["ms"].at[k, e], R["mr"].at[k, e], peer_of(e)) for e in order]

    def small_sum(k, cps, order, buf, nxt):
        s = mt[k]
        for e, cp in zip(order, cps):
            cp.wait_recv()
            s = s + buf[e]
        mt[nxt] = s

    def y1_rows(k):
        rr = rows(k, XN * BLK)
        v = jnp.dot(xg[rr, :], b1, preferred_element_type=F32).astype(BF)
        for j in range(XN):
            yg[0, pl.ds(pl.multiple_of((k * XN + j) * 128 + mine_at, BLK), BLK), :] = v[j * BLK:(j + 1) * BLK]

    def y2_rows(k):
        unpack_rows(y2g, k * XN, XN, yg.at[1], 128, mine_at)

    mzc = exchange_small(0, mt.at[0], R["mz"], z_order, lambda e: dev(dz=e))
    fwd_gather(0, xg, BLK, y1_rows, lambda s: None, False)
    small_sum(0, mzc, z_order, R["mz"], 1)
    mxc = exchange_small(1, mt.at[1], R["mx"], x_order, lambda e: dev(dx=e))
    z1 = fwd_reduce(0, False, 14)
    R["z1s"][...] = z1
    h1 = jnp.maximum(z1, 0.0).astype(BF)
    R["h1s"][...] = h1
    nt = (((1,), (1,)), ((), ()))
    y2 = lax.dot_general(h1, w2p[...], nt, preferred_element_type=F32)
    y2g[rows(own_f, PB), :] = pack(y2).astype(BF)
    small_sum(1, mxc, x_order, R["mx"], 2)
    myc = exchange_small(2, mt.at[2], R["my"], y_order, lambda e: dev(dy=e))
    fwd_gather(1, y2g, PB, y2_rows, fill_hook, False)
    small_sum(2, myc, y_order, R["my"], 3)
    mcc = exchange_small(3, mt.at[3], R["mc"], [1], lambda e: dev(dc=e))
    z2 = fwd_reduce(1, True, 99)
    small_sum(3, mcc, [1], R["mc"], 4)

    count = mt[4][:1, :1]
    diag = lax.broadcasted_iota(jnp.int32, (BLK, BLK), 0) == lax.broadcasted_iota(jnp.int32, (BLK, BLK), 1)
    labf = jnp.sum(jnp.where(diag, jnp.broadcast_to(R["lab"][...].astype(F32), (BLK, BLK)), 0.0), axis=1, keepdims=True)
    mskf = jnp.sum(jnp.where(diag, jnp.broadcast_to(mask_row, (BLK, BLK)), 0.0), axis=1, keepdims=True)
    lane = lax.broadcasted_iota(jnp.int32, z2.shape, 1)
    logits = jnp.where(lane < classes, z2, NEG)
    shifted = logits - jnp.max(logits, axis=1, keepdims=True)
    log_probs = shifted - jnp.log(jnp.sum(jnp.exp(shifted), axis=1, keepdims=True))
    onehot = jnp.where(lane.astype(F32) == labf, 1.0, 0.0)
    g2 = (jnp.exp(log_probs) - onehot) * (mskf / count)
    g2g[rows(r, PB), :] = pack(g2).astype(BF)
    local_loss = -jnp.sum(mskf * jnp.sum(onehot * log_probs, axis=1, keepdims=True), axis=0, keepdims=True)

    dacc = R["dacc"]

    def bwd(g, buf, size, packed, hooks, late=lambda: None):
        gu = R["gu"] if packed else buf

        def done(zk, k):
            if packed:
                unpack_rows(buf, zk * YN, YN, gu)
            rr = rows(zk, YN * BLK)
            v = jnp.dot(at[:, rr], gu[rr, :], preferred_element_type=F32)
            if k == 0:
                dacc[...] = v
            else:
                dacc[...] += v

        gather(g, buf, lambda zk, yk: zk * YN + yk, size, YN, y, lambda e: dev(dy=e), done, hooks)
        dp, dr, dsum, dx = (R["dpp"], R["drp"], R["dsp"], R["dxp"]) if packed else (R["dp"], R["dr"], R["ds"], R["dx"])
        for k in range(2):
            for j in range(XN):
                piece = dacc[(k * XN + j) * BLK:(k * XN + j + 1) * BLK]
                dp[k, j] = pack(piece) if packed else piece
        cp = send(dp.at[1 - c], dr, R["cs"].at[g, 0], R["cr"].at[g, 0], dev(dc=1))
        cp.wait_recv()
        dsum[...] = dp[c] + dr[...]
        cps = [send(dsum.at[lax.rem(x + e, XN)], dx.at[e], R["rs"].at[g, e], R["rr"].at[g, e], dev(dx=e)) for e in x_order]
        late()
        drain(len(cps) + 3)
        total = dsum[x]
        for e, cp in zip(x_order, cps):
            cp.wait_recv()
            total = total + dx[e]
        return (unpack(total) if packed else total).astype(BF)

    def all_reduce(t, pay, payx, payy, payz, fin, whole):
        rx = pay.shape[0] // node_n
        ry = rx // YN
        fs, fr = R["fs"], R["fr"]
        state = {}
        others = range(1, node_n)
        small = pl.ds(pl.multiple_of(i * rx + y * ry, 8), ry)

        def total(first, buf, order):
            for e, cp in zip(order, state["cp"]):
                cp.wait_recv()
                first = first + buf[e]
            return first

        def s0():
            state["cp"] = [send(pay.at[rows(lax.rem(i + e, node_n), rx)], payx.at[e], fs.at[t, 0, e], fr.at[t, 0, e], node_dev(e)) for e in others]

        def w1():
            payy[y] = total(pay[rows(i, rx)], payx, others)
            state["cp"] = [send(payy.at[y], payy.at[y], fs.at[t, 1, e], fr.at[t, 1, e], dev(dy=e)) for e in y_order]

        def in_order(buf, n):
            for cp in state["cp"]:
                cp.wait_recv()
            s = buf[0]
            for k in range(1, n):
                s = s + buf[k]
            return s

        def w2():
            payz[z] = in_order(payy, YN)
            state["cp"] = [send(payz.at[z], payz.at[z], fs.at[t, 2, d], fr.at[t, 2, d], dev(dz=d)) for d in z_order]

        def w3():
            fin[rows(i, rx)] = in_order(payz, ZN)
            mine = fin.at[rows(i, rx)]
            state["cp"] = [send(mine, mine, fs.at[t, 4, e], fr.at[t, 4, e], node_dev(e)) for e in others]

        def s1():
            payx[0] = total(pay[rows(i, rx)], payx, others)
            state["cp"] = [send(payx.at[0, rows(lax.rem(y + e, YN), ry)], payy.at[e], fs.at[t, 1, e], fr.at[t, 1, e], dev(dy=e)) for e in y_order]

        def s2():
            payz[z] = total(payx[0, rows(y, ry)], payy, y_order)
            state["cp"] = [send(payz.at[z], payz.at[z], fs.at[t, 2, d], fr.at[t, 2, d], dev(dz=d)) for d in z_order]

        def s3():
            for cp in state["cp"]:
                cp.wait_recv()
            s = payz[0]
            for k in range(1, ZN):
                s = s + payz[k]
            fin[small] = s
            state["cp"] = [send(fin.at[small], fin.at[small], fs.at[t, 3, e], fr.at[t, 3, e], dev(dy=e)) for e in y_order]

        def s4():
            for cp in state["cp"]:
                cp.wait_recv()
            mine = fin.at[rows(i, rx)]
            state["cp"] = [send(mine, mine, fs.at[t, 4, e], fr.at[t, 4, e], node_dev(e)) for e in others]

        def s5():
            for cp in state["cp"]:
                cp.wait_recv()

        return [s0, w1, w2, w3, s5] if whole else [s0, s1, s2, s3, s4, s5]

    d2 = bwd(2, g2g, PB, True, lambda s: None)
    tn = (((0,), (0,)), ((), ()))
    dh1 = jnp.dot(d2, w2p[...], preferred_element_type=F32)
    g1g[rows(r, BLK), :] = jnp.where(R["z1s"][...] > 0, dh1, 0.0).astype(BF)
    R["d2s"][...] = d2
    ar2 = all_reduce(0, R["pay2"], R["payx2"], R["payy2"], R["payz2"], R["fin2"], False)

    def make_dw2():
        dw2 = lax.dot_general(R["d2s"][...], R["h1s"][...], tn, preferred_element_type=F32)
        row = lax.broadcasted_iota(jnp.int32, (256, 128), 0)
        lane2 = lax.broadcasted_iota(jnp.int32, (256, 128), 1)
        R["pay2"][0:256] = jnp.where(jnp.logical_and(row == 255, lane2 == 127), local_loss, dw2[:, :128])
        R["pay2"][256:512] = dw2[:, 128:]
        ar2[0]()

    def beside_hook(s):
        if s == 0:
            make_dw2()

    d1 = bwd(3, g1g, BLK, False, beside_hook, ar2[1])
    dw1 = lax.dot_general(x_ref[...], d1, tn, preferred_element_type=F32)
    R["pay1"][0:f_in] = dw1[:, :128]
    R["pay1"][f_in:2 * f_in] = dw1[:, 128:]
    ar1 = all_reduce(1, R["pay1"], R["payx1"], R["payy1"], R["payz1"], R["fin1"], True)
    for s in range(5):
        ar1[s]()
        if s < 4:
            ar2[2 + s]()
    R["o1"][...] = R["fin1"][...]
    R["o2"][...] = R["fin2"][...]
    R["cnt"][...] = mt[4]
    for cp in pending:
        cp.wait_send()


def write_outputs(fin1, fin2, count, loss_ref, dw1_ref, dw2_ref):
    f_in, classes = dw1_ref.shape[0], dw2_ref.shape[0]
    dw2_ref[:, :128] = fin2[0:classes]
    dw2_ref[:, 128:] = fin2[256:256 + classes]
    loss_ref[0, 0] = jnp.sum(fin2[255:256, 127:] / count[:1, :1])
    dw1_ref[:, :128] = fin1[0:f_in]
    dw1_ref[:, 128:] = fin1[f_in:2 * f_in]


def solution(mesh):
    rep_n, node_n = mesh.shape["rep"], mesh.shape["nodes"]
    YN = 4
    ZN = rep_n // YN
    XN = node_n // 2

    def local_step(adj, features, w_one, w_two, labels, mask):
        f_in, hidden = w_one.shape
        classes = w_two.shape[1]
        rows_g = adj.shape[0]
        blocks_y = node_n * ZN
        V = pltpu.VMEM
        D = pltpu.SemaphoreType.DMA

        def reduce_bufs(t, n, cut):
            rx = n // node_n
            return {f"pay{t}": V((n, 128), F32), f"payx{t}": V((node_n, rx, 128), F32),
                    f"payy{t}": V((YN, rx // cut, 128), F32), f"payz{t}": V((ZN, rx // cut, 128), F32), f"fin{t}": V((n, 128), F32)}

        scratch = dict(
            af=V((YN * BLK, blocks_y * 128), BF),
            ab=V((node_n, rows_g, 128), BF), at=V((node_n * BLK, rows_g), BF),
            xg=V((blocks_y * BLK, f_in), BF), yg=V((2, blocks_y * 128, 256), BF), y2g=V((blocks_y * 96, 128), BF),
            g2g=V((rep_n * 96, 128), BF), gu=V((rows_g, 256), BF), g1g=V((rows_g, hidden), BF),
            zacc=V((YN * BLK, 256), F32), dacc=V((node_n * BLK, 256), F32),
            zp=V((YN, BLK, 256), F32), zrw=V((YN, BLK, 256), F32), zpp=V((YN, 96, 128), F32), zrp=V((YN, 96, 128), F32),
            dp=V((2, XN, BLK, 256), F32), dr=V((XN, BLK, 256), F32), ds=V((XN, BLK, 256), F32), dx=V((XN, BLK, 256), F32),
            dpp=V((2, XN, 96, 128), F32), drp=V((XN, 96, 128), F32), dsp=V((XN, 96, 128), F32), dxp=V((XN, 96, 128), F32),
            mt=V((5, 8, 128), F32), mz=V((ZN, 8, 128), F32), mx=V((XN, 8, 128), F32), my=V((YN, 8, 128), F32),
            mc=V((2, 8, 128), F32),
            z1s=V((BLK, hidden), F32), h1s=V((BLK, hidden), BF), d2s=V((BLK, 256), BF), w2p=V((256, hidden), BF),
            sem_af=D, sem_ab=D,
            zs=D((4, 8)), zr=D((4, 8)), ss=D((4, 8, 4)), sr=D((4, 8, 4)), cs=D((4, 8)), cr=D((4, 8)),
            rs=D((4, 4)), rr=D((4, 4)), ms=D((4, 8)), mr=D((4, 8)), fs=D((2, 7, 8)), fr=D((2, 7, 8)),
        )
        scratch.update(reduce_bufs(1, 2 * f_in, 1))
        scratch.update(reduce_bufs(2, 512, YN))
        names = ["a", "x", "w1", "w2", "lab", "msk", "o1", "o2", "cnt"] + list(scratch)
        vm = pl.BlockSpec(memory_space=pltpu.VMEM)
        sums = pl.pallas_call(
            functools.partial(step_kernel, ZN, YN, XN, names),
            out_shape=(jax.ShapeDtypeStruct((2 * f_in, 128), F32), jax.ShapeDtypeStruct((512, 128), F32),
                       jax.ShapeDtypeStruct((8, 128), F32)),
            in_specs=[pl.BlockSpec(memory_space=pl.ANY), vm, vm, vm, vm, vm],
            out_specs=(vm, vm, vm),
            scratch_shapes=list(scratch.values()),
            compiler_params=pltpu.CompilerParams(collective_id=0, has_side_effects=True, vmem_limit_bytes=60 * 2 ** 20),
            name="gcn_step",
        )(adj, features, w_one, w_two.T, labels.reshape(1, BLK), mask.reshape(1, BLK))
        loss, dw1, dw2 = pl.pallas_call(
            write_outputs,
            out_shape=(jax.ShapeDtypeStruct((1, 1), F32), jax.ShapeDtypeStruct((f_in, hidden), F32),
                       jax.ShapeDtypeStruct((classes, hidden), F32)),
            in_specs=[vm, vm, vm],
            out_specs=(pl.BlockSpec(memory_space=pltpu.SMEM), vm, vm),
            name="write_outputs",
        )(*sums)
        return loss.reshape(()), dw1, dw2.T

    row_spec = P(("nodes", "rep"))
    return jax.shard_map(local_step, mesh=mesh, in_specs=(P("nodes", None), P(("nodes", "rep"), None), P(), P(), row_spec, row_spec),
                         out_specs=(P(), P(), P()), check_vma=False)
```

```python
import functools

import jax
import jax.numpy as jnp
from jax import lax
from jax.experimental import pallas as pl
from jax.experimental.pallas import tpu as pltpu
from jax.sharding import PartitionSpec as P

BF = jnp.bfloat16
F32 = jnp.float32
BLK = 64
NEG = -1e30


def ring_order(n):
    return sorted(range(1, n), key=lambda d: (min(d, n - d), d))


def pack(v):
    out = []
    lane = lax.broadcasted_iota(jnp.int32, (BLK // 2, 128), 1)
    for k in range(v.shape[0] // BLK):
        lo, hi = v[k * BLK:(k + 1) * BLK, :128], v[k * BLK:(k + 1) * BLK, 128:]
        out += [lo, jnp.where(lane < 64, hi[:BLK // 2], pltpu.roll(hi[BLK // 2:], 64, 1))]
    return jnp.concatenate(out, axis=0)


def unpack(p):
    lane = lax.broadcasted_iota(jnp.int32, (BLK // 2, 128), 1)
    t = p[BLK:]
    hi = jnp.concatenate([jnp.where(lane < 64, t, 0.0), jnp.where(lane < 64, pltpu.roll(t, 64, 1), 0.0)], axis=0)
    return jnp.concatenate([p[:BLK], hi], axis=1)


def step_kernel(ZN, YN, XN, names, *refs):
    R = dict(zip(names, refs))
    a_hbm, x_ref, w1_ref, w2_ref = R["a"], R["x"], R["w1"], R["w2"]
    af, ab, at, w2p, mt = R["af"], R["ab"], R["at"], R["w2p"], R["mt"]
    rep_n, node_n = ZN * YN, 2 * XN
    r, i = lax.axis_index("rep"), lax.axis_index("nodes")
    z, y = r // YN, lax.rem(r, YN)
    x, c = i // 2, lax.rem(i, 2)
    classes, hidden = w2_ref.shape
    f_in = x_ref.shape[1]
    PB = 96

    def dev(dz=0, dy=0, dx=0, dc=0):
        return {"rep": lax.rem(z + dz, ZN) * YN + lax.rem(y + dy, YN),
                "nodes": lax.rem(x + dx, XN) * 2 + lax.rem(c + dc, 2)}

    def node_dev(e):
        return {"rep": r, "nodes": lax.rem(i + e, node_n)}

    def rows(k, n):
        return pl.ds(pl.multiple_of(k * n, n), n)

    z_order, y_order, x_order = ring_order(ZN), ring_order(YN), ring_order(XN)
    peers = [dev(dz=d) for d in z_order] + [dev(dy=d) for d in y_order] + [node_dev(e) for e in range(1, node_n)]

    rows_z = YN * BLK
    n_q = node_n * ZN

    @pl.loop(0, n_q)
    def _(q):
        pltpu.make_async_copy(
            a_hbm.at[rows(z, rows_z), pl.ds(pl.multiple_of(q * (YN * BLK) + (y // 2) * 128, 128), 128)],
            af.at[:, rows((lax.rem(q // ZN, 2) * ZN + lax.rem(q, ZN)) * XN + q // (2 * ZN), 128)], R["sem_af"]).start()

    barrier = pltpu.get_barrier_semaphore()
    for peer in peers:
        pl.semaphore_signal(barrier, inc=1, device_id=peer, device_id_type=pl.DeviceIdType.MESH)

    xg, yg, y2g, g2g, g1g = R["xg"], R["yg"], R["y2g"], R["g2g"], R["g1g"]
    own_f = (c * ZN + z) * XN + x
    xg[rows(own_f, BLK), :] = x_ref[...]
    mine_at = lax.rem(y, 2) * BLK

    @pl.loop(0, yg.shape[1] // 128)
    def _(k):
        zero_rows = pl.ds(pl.multiple_of(k * 128 + BLK - mine_at, BLK), BLK)
        for t in range(2):
            yg[t, zero_rows, :] = jnp.zeros((BLK, 256), BF)

    w2p[...] = jnp.zeros_like(w2p)
    w2p[:classes, :] = w2_ref[...].astype(BF)
    b1 = w1_ref[...].astype(BF)
    mask_row = R["msk"][...].astype(F32)
    mt[0] = jnp.broadcast_to(jnp.sum(mask_row, axis=1, keepdims=True), mt.shape[1:])

    pl.semaphore_wait(barrier, len(peers))

    pending = []

    def drain(keep):
        while len(pending) > keep:
            pending.pop(0).wait_send()

    def send(src, dst, ssem, rsem, device):
        cp = pltpu.make_async_remote_copy(src_ref=src, dst_ref=dst, send_sem=ssem, recv_sem=rsem,
                                          device_id=device, device_id_type=pl.DeviceIdType.MESH)
        cp.start()
        pending.append(cp)
        return cp

    def gather(g, buf, index, size, n, me, peer_of, done, hooks):
        zs, zr, ss, sr = R["zs"], R["zr"], R["ss"], R["sr"]

        def slot(zk):
            return buf.at[rows(index(zk, me), size)]

        def zof(k):
            return lax.rem(z + ZN - k, ZN)

        line = {}
        early = [k for k in [0] + z_order if min(k, ZN - k) <= 2] if n == 4 else []

        def spread(k):
            mine = slot(zof(k))
            line[k] = [send(mine, mine, ss.at[g, k, e], sr.at[g, k, e], peer_of(e))
                       for e in ring_order(n) if e != 2 or k not in early]

        def relay(k):
            far = []
            for h, cp in enumerate(line[k]):
                cp.wait_recv()
                at_row = index(zof(k), lax.rem(me + (n - 1 if h == 0 else 1), n)) * size + h * (size // 2)
                piece = buf.at[pl.ds(pl.multiple_of(at_row, size // 2), size // 2)]
                far.append(send(piece, piece, ss.at[g, k, 2 * h], sr.at[g, k, 2 * h], peer_of(1 if h == 0 else n - 1)))
            line[k] = far

        zc = {d: send(slot(z), slot(z), zs.at[g, d], zr.at[g, d], dev(dz=d)) for d in z_order[:2]}
        spread(0)
        zc.update({d: send(slot(z), slot(z), zs.at[g, d], zr.at[g, d], dev(dz=d)) for d in z_order[2:]})
        after = {1: "r0", 3: "r1 r7", 5: "l0 r2 r6", 6: "l1 l7 l2 l6 l3 l5 l4"} if ZN == 8 else {ZN - 2: "r0 l0 r1 l1"}
        events = []
        for s, d in enumerate(z_order):
            events.append(("z", d))
            events += [(w[0], int(w[1:])) for w in after.get(s, "").split() if w[0] == "l" or int(w[1:]) in early]
        for s, (what, k) in enumerate(events):
            hooks(s if what != "r" else 99)
            if what == "z":
                zc[k].wait_recv()
                spread(k)
            elif what == "r":
                relay(k)
            else:
                for cp in line[k]:
                    cp.wait_recv()
                done(zof(k), k)

    def start_ab():
        @pl.loop(0, node_n)
        def _(j):
            pltpu.make_async_copy(
                a_hbm.at[:, pl.ds(pl.multiple_of(j * (rep_n * BLK) + (r // 2) * 128, 128), 128)],
                ab.at[j], R["sem_ab"]).start()

    TR = min(512, at.shape[1])

    def transpose_part(j, q):
        if j == q == 0:
            pltpu.make_async_copy(ab, ab, R["sem_ab"]).wait()
        t = ab[(j % XN) * 2 + j // XN, q * TR:(q + 1) * TR, :].T

        @pl.when(lax.rem(r, 2) == 0)
        def _():
            at[j * BLK:(j + 1) * BLK, q * TR:(q + 1) * TR] = t[:BLK]

        @pl.when(lax.rem(r, 2) == 1)
        def _():
            at[j * BLK:(j + 1) * BLK, q * TR:(q + 1) * TR] = t[BLK:]

    fillers = [functools.partial(transpose_part, j, q) for j in range(node_n) for q in range(at.shape[1] // TR)]

    def fill(n):
        for _ in range(min(n, len(fillers))):
            fillers.pop(0)()

    def fill_hook(s):
        if s < 14:
            fill(1)

    def unpack_rows(buf, first_block, n, out, pitch=BLK, shift=0):
        for k in range(n):
            base = pl.multiple_of((first_block + k) * PB, 32)
            orow = pl.multiple_of((first_block + k) * pitch + shift, BLK)
            t = buf[pl.ds(base + BLK, BLK // 2), :]
            out[pl.ds(orow, BLK), :128] = buf[pl.ds(base, BLK), :]
            out[pl.ds(orow, BLK // 2), 128:] = t
            out[pl.ds(orow + BLK // 2, BLK // 2), 128:] = jnp.concatenate([t[:, 64:], t[:, :64]], axis=1)

    zacc = R["zacc"]

    def fwd_gather(g, buf, size, prepare, hooks):
        late = []

        def line(ck, zk):
            return buf.at[rows(ck * ZN + zk, XN * size)]

        def add(ck, zk, first):
            k = ck * ZN + zk
            if first and g == 0:
                pltpu.make_async_copy(af, af, R["sem_af"]).wait()
                start_ab()
            prepare(k)
            v = jnp.dot(af[:, rows(k, XN * 128)], yg[g, rows(k, XN * 128), :], preferred_element_type=F32)
            if first:
                zacc[...] = v
            else:
                zacc[...] += v

        def partner():
            cp, zk = late.pop(0)
            cp.wait_recv()
            add(1 - c, zk, False)

        def done(zk, k):
            mine = line(c, zk)
            late.append((send(mine, mine, R["cs"].at[g, k], R["cr"].at[g, k], dev(dc=1)), zk))
            add(c, zk, k == 0)
            if len(late) > 2:
                partner()

        gather(g, buf, lambda zk, xk: (c * ZN + zk) * XN + xk, size, XN, x, lambda e: dev(dx=e), done, hooks)
        while late:
            partner()

    def fwd_reduce(g, packed, n_fill):
        zp, zr = (R["zpp"], R["zrp"]) if packed else (R["zp"], R["zrw"])
        v = zacc[...]
        for k in range(YN):
            piece = v[k * BLK:(k + 1) * BLK]
            zp[k] = pack(piece) if packed else piece
        cps = [send(zp.at[lax.rem(y + e, YN)], zr.at[e], R["rs"].at[g, e], R["rr"].at[g, e], dev(dy=e)) for e in y_order]
        fill(n_fill)
        drain(len(cps))
        total = zp[y]
        for e, cp in zip(y_order, cps):
            cp.wait_recv()
            total = total + zr[e]
        return unpack(total) if packed else total

    def exchange_small(k, src, buf, order, peer_of):
        return [send(src, buf.at[e], R["ms"].at[k, e], R["mr"].at[k, e], peer_of(e)) for e in order]

    def small_sum(k, cps, order, buf, nxt):
        s = mt[k]
        for e, cp in zip(order, cps):
            cp.wait_recv()
            s = s + buf[e]
        mt[nxt] = s

    def y1_rows(k):
        rr = rows(k, XN * BLK)
        v = jnp.dot(xg[rr, :], b1, preferred_element_type=F32).astype(BF)
        for j in range(XN):
            yg[0, pl.ds(pl.multiple_of((k * XN + j) * 128 + mine_at, BLK), BLK), :] = v[j * BLK:(j + 1) * BLK]

    def y2_rows(k):
        unpack_rows(y2g, k * XN, XN, yg.at[1], 128, mine_at)

    mzc = []

    def count_hook(s):
        if s == 0:
            mzc.extend(exchange_small(0, mt.at[0], R["mz"], z_order, lambda e: dev(dz=e)))

    fwd_gather(0, xg, BLK, y1_rows, count_hook)
    small_sum(0, mzc, z_order, R["mz"], 1)
    mxc = exchange_small(1, mt.at[1], R["mx"], x_order, lambda e: dev(dx=e))
    z1 = fwd_reduce(0, False, 12)
    R["z1s"][...] = z1
    h1 = jnp.maximum(z1, 0.0).astype(BF)
    R["h1s"][...] = h1
    nt = (((1,), (1,)), ((), ()))
    y2 = lax.dot_general(h1, w2p[...], nt, preferred_element_type=F32)
    y2g[rows(own_f, PB), :] = pack(y2).astype(BF)
    small_sum(1, mxc, x_order, R["mx"], 2)
    myc = exchange_small(2, mt.at[2], R["my"], y_order, lambda e: dev(dy=e))
    fwd_gather(1, y2g, PB, y2_rows, fill_hook)
    small_sum(2, myc, y_order, R["my"], 3)
    mcc = exchange_small(3, mt.at[3], R["mc"], [1], lambda e: dev(dc=e))
    z2 = fwd_reduce(1, True, 99)
    small_sum(3, mcc, [1], R["mc"], 4)

    count = mt[4][:1, :1]
    diag = lax.broadcasted_iota(jnp.int32, (BLK, BLK), 0) == lax.broadcasted_iota(jnp.int32, (BLK, BLK), 1)
    labf = jnp.sum(jnp.where(diag, jnp.broadcast_to(R["lab"][...].astype(F32), (BLK, BLK)), 0.0), axis=1, keepdims=True)
    mskf = jnp.sum(jnp.where(diag, jnp.broadcast_to(mask_row, (BLK, BLK)), 0.0), axis=1, keepdims=True)
    lane = lax.broadcasted_iota(jnp.int32, z2.shape, 1)
    logits = jnp.where(lane < classes, z2, NEG)
    shifted = logits - jnp.max(logits, axis=1, keepdims=True)
    log_probs = shifted - jnp.log(jnp.sum(jnp.exp(shifted), axis=1, keepdims=True))
    onehot = jnp.where(lane.astype(F32) == labf, 1.0, 0.0)
    g2 = (jnp.exp(log_probs) - onehot) * (mskf / count)
    g2g[rows(r, PB), :] = pack(g2).astype(BF)
    local_loss = -jnp.sum(mskf * jnp.sum(onehot * log_probs, axis=1, keepdims=True), axis=0, keepdims=True)

    dacc = R["dacc"]

    def bwd(g, buf, size, packed, hooks, late=lambda: None):
        gu = R["gu"] if packed else buf

        def done(zk, k):
            if packed:
                unpack_rows(buf, zk * YN, YN, gu)
            rr = rows(zk, YN * BLK)
            v = jnp.dot(at[:, rr], gu[rr, :], preferred_element_type=F32)
            if k == 0:
                dacc[...] = v
            else:
                dacc[...] += v

        gather(g, buf, lambda zk, yk: zk * YN + yk, size, YN, y, lambda e: dev(dy=e), done, hooks)
        dp, dr, dsum, dx = (R["dpp"], R["drp"], R["dsp"], R["dxp"]) if packed else (R["dp"], R["dr"], R["ds"], R["dx"])
        for k in range(2):
            for j in range(XN):
                piece = dacc[(k * XN + j) * BLK:(k * XN + j + 1) * BLK]
                dp[k, j] = pack(piece) if packed else piece
        cp = send(dp.at[1 - c], dr, R["cs"].at[g, 0], R["cr"].at[g, 0], dev(dc=1))
        cp.wait_recv()
        dsum[...] = dp[c] + dr[...]
        cps = [send(dsum.at[lax.rem(x + e, XN)], dx.at[e], R["rs"].at[g, e], R["rr"].at[g, e], dev(dx=e)) for e in x_order]
        late()
        drain(len(cps) + 3)
        total = dsum[x]
        for e, cp in zip(x_order, cps):
            cp.wait_recv()
            total = total + dx[e]
        return (unpack(total) if packed else total).astype(BF)

    def all_reduce(t, pay, payx, payy, payz, fin, whole):
        rx = pay.shape[0] // node_n
        ry = rx // YN
        fs, fr = R["fs"], R["fr"]
        state = {}
        others = range(1, node_n)
        small = pl.ds(pl.multiple_of(i * rx + y * ry, 8), ry)

        def total(first, buf, order):
            for e, cp in zip(order, state["cp"]):
                cp.wait_recv()
                first = first + buf[e]
            return first

        def s0():
            state["cp"] = [send(pay.at[rows(lax.rem(i + e, node_n), rx)], payx.at[e], fs.at[t, 0, e], fr.at[t, 0, e], node_dev(e)) for e in others]

        def w1():
            payy[y] = total(pay[rows(i, rx)], payx, others)
            state["cp"] = [send(payy.at[y], payy.at[y], fs.at[t, 1, e], fr.at[t, 1, e], dev(dy=e)) for e in y_order]

        def in_order(buf, n):
            for cp in state["cp"]:
                cp.wait_recv()
            s = buf[0]
            for k in range(1, n):
                s = s + buf[k]
            return s

        def w2():
            payz[z] = in_order(payy, YN)
            state["cp"] = [send(payz.at[z], payz.at[z], fs.at[t, 2, d], fr.at[t, 2, d], dev(dz=d)) for d in z_order]

        def w3():
            fin[rows(i, rx)] = in_order(payz, ZN)
            mine = fin.at[rows(i, rx)]
            state["cp"] = [send(mine, mine, fs.at[t, 4, e], fr.at[t, 4, e], node_dev(e)) for e in others]

        def s1():
            payx[0] = total(pay[rows(i, rx)], payx, others)
            state["cp"] = [send(payx.at[0, rows(lax.rem(y + e, YN), ry)], payy.at[e], fs.at[t, 1, e], fr.at[t, 1, e], dev(dy=e)) for e in y_order]

        def s2():
            payz[z] = total(payx[0, rows(y, ry)], payy, y_order)
            state["cp"] = [send(payz.at[z], payz.at[z], fs.at[t, 2, d], fr.at[t, 2, d], dev(dz=d)) for d in z_order]

        def s3():
            for cp in state["cp"]:
                cp.wait_recv()
            s = payz[0]
            for k in range(1, ZN):
                s = s + payz[k]
            fin[small] = s
            state["cp"] = [send(fin.at[small], fin.at[small], fs.at[t, 3, e], fr.at[t, 3, e], dev(dy=e)) for e in y_order]

        def s4():
            for cp in state["cp"]:
                cp.wait_recv()
            mine = fin.at[rows(i, rx)]
            state["cp"] = [send(mine, mine, fs.at[t, 4, e], fr.at[t, 4, e], node_dev(e)) for e in others]

        def s5():
            for cp in state["cp"]:
                cp.wait_recv()

        return [s0, w1, w2, w3, s5] if whole else [s0, s1, s2, s3, s4, s5]

    d2 = bwd(2, g2g, PB, True, lambda s: None)
    tn = (((0,), (0,)), ((), ()))
    dh1 = jnp.dot(d2, w2p[...], preferred_element_type=F32)
    g1g[rows(r, BLK), :] = jnp.where(R["z1s"][...] > 0, dh1, 0.0).astype(BF)
    R["d2s"][...] = d2
    ar2 = all_reduce(0, R["pay2"], R["payx2"], R["payy2"], R["payz2"], R["fin2"], False)

    def make_dw2():
        dw2 = lax.dot_general(R["d2s"][...], R["h1s"][...], tn, preferred_element_type=F32)
        row = lax.broadcasted_iota(jnp.int32, (256, 128), 0)
        lane2 = lax.broadcasted_iota(jnp.int32, (256, 128), 1)
        R["pay2"][0:256] = jnp.where(jnp.logical_and(row == 255, lane2 == 127), local_loss, dw2[:, :128])
        R["pay2"][256:512] = dw2[:, 128:]
        ar2[0]()

    def beside_hook(s):
        if s == 0:
            make_dw2()

    d1 = bwd(3, g1g, BLK, False, beside_hook, ar2[1])
    dw1 = lax.dot_general(x_ref[...], d1, tn, preferred_element_type=F32)
    R["pay1"][0:f_in] = dw1[:, :128]
    R["pay1"][f_in:2 * f_in] = dw1[:, 128:]
    ar1 = all_reduce(1, R["pay1"], R["payx1"], R["payy1"], R["payz1"], R["fin1"], True)
    for s in range(5):
        ar1[s]()
        if s < 4:
            ar2[2 + s]()
    R["o1"][...] = R["fin1"][...]
    R["o2"][...] = R["fin2"][...]
    R["cnt"][...] = mt[4]
    for cp in pending:
        cp.wait_send()


def write_outputs(fin1, fin2, count, loss_ref, dw1_ref, dw2_ref):
    f_in, classes = dw1_ref.shape[0], dw2_ref.shape[0]
    dw2_ref[:, :128] = fin2[0:classes]
    dw2_ref[:, 128:] = fin2[256:256 + classes]
    loss_ref[0, 0] = jnp.sum(fin2[255:256, 127:] / count[:1, :1])
    dw1_ref[:, :128] = fin1[0:f_in]
    dw1_ref[:, 128:] = fin1[f_in:2 * f_in]


def solution(mesh):
    rep_n, node_n = mesh.shape["rep"], mesh.shape["nodes"]
    YN = 4
    ZN = rep_n // YN
    XN = node_n // 2

    def local_step(adj, features, w_one, w_two, labels, mask):
        f_in, hidden = w_one.shape
        classes = w_two.shape[1]
        rows_g = adj.shape[0]
        blocks_y = node_n * ZN
        V = pltpu.VMEM
        D = pltpu.SemaphoreType.DMA

        def reduce_bufs(t, n, cut):
            rx = n // node_n
            return {f"pay{t}": V((n, 128), F32), f"payx{t}": V((node_n, rx, 128), F32),
                    f"payy{t}": V((YN, rx // cut, 128), F32), f"payz{t}": V((ZN, rx // cut, 128), F32), f"fin{t}": V((n, 128), F32)}

        scratch = dict(
            af=V((YN * BLK, blocks_y * 128), BF),
            ab=V((node_n, rows_g, 128), BF), at=V((node_n * BLK, rows_g), BF),
            xg=V((blocks_y * BLK, f_in), BF), yg=V((2, blocks_y * 128, 256), BF), y2g=V((blocks_y * 96, 128), BF),
            g2g=V((rep_n * 96, 128), BF), gu=V((rows_g, 256), BF), g1g=V((rows_g, hidden), BF),
            zacc=V((YN * BLK, 256), F32), dacc=V((node_n * BLK, 256), F32),
            zp=V((YN, BLK, 256), F32), zrw=V((YN, BLK, 256), F32), zpp=V((YN, 96, 128), F32), zrp=V((YN, 96, 128), F32),
            dp=V((2, XN, BLK, 256), F32), dr=V((XN, BLK, 256), F32), ds=V((XN, BLK, 256), F32), dx=V((XN, BLK, 256), F32),
            dpp=V((2, XN, 96, 128), F32), drp=V((XN, 96, 128), F32), dsp=V((XN, 96, 128), F32), dxp=V((XN, 96, 128), F32),
            mt=V((5, 8, 128), F32), mz=V((ZN, 8, 128), F32), mx=V((XN, 8, 128), F32), my=V((YN, 8, 128), F32),
            mc=V((2, 8, 128), F32),
            z1s=V((BLK, hidden), F32), h1s=V((BLK, hidden), BF), d2s=V((BLK, 256), BF), w2p=V((256, hidden), BF),
            sem_af=D, sem_ab=D,
            zs=D((4, 8)), zr=D((4, 8)), ss=D((4, 8, 4)), sr=D((4, 8, 4)), cs=D((4, 8)), cr=D((4, 8)),
            rs=D((4, 4)), rr=D((4, 4)), ms=D((4, 8)), mr=D((4, 8)), fs=D((2, 7, 8)), fr=D((2, 7, 8)),
        )
        scratch.update(reduce_bufs(1, 2 * f_in, 1))
        scratch.update(reduce_bufs(2, 512, YN))
        names = ["a", "x", "w1", "w2", "lab", "msk", "o1", "o2", "cnt"] + list(scratch)
        vm = pl.BlockSpec(memory_space=pltpu.VMEM)
        sums = pl.pallas_call(
            functools.partial(step_kernel, ZN, YN, XN, names),
            out_shape=(jax.ShapeDtypeStruct((2 * f_in, 128), F32), jax.ShapeDtypeStruct((512, 128), F32),
                       jax.ShapeDtypeStruct((8, 128), F32)),
            in_specs=[pl.BlockSpec(memory_space=pl.ANY), vm, vm, vm, vm, vm],
            out_specs=(vm, vm, vm),
            scratch_shapes=list(scratch.values()),
            compiler_params=pltpu.CompilerParams(collective_id=0, has_side_effects=True, vmem_limit_bytes=60 * 2 ** 20),
            name="gcn_step",
        )(adj, features, w_one, w_two.T, labels.reshape(1, BLK), mask.reshape(1, BLK))
        loss, dw1, dw2 = pl.pallas_call(
            write_outputs,
            out_shape=(jax.ShapeDtypeStruct((1, 1), F32), jax.ShapeDtypeStruct((f_in, hidden), F32),
                       jax.ShapeDtypeStruct((classes, hidden), F32)),
            in_specs=[vm, vm, vm],
            out_specs=(pl.BlockSpec(memory_space=pltpu.SMEM), vm, vm),
            name="write_outputs",
        )(*sums)
        return loss.reshape(()), dw1, dw2.T

    row_spec = P(("nodes", "rep"))
    return jax.shard_map(local_step, mesh=mesh, in_specs=(P("nodes", None), P(("nodes", "rep"), None), P(), P(), row_spec, row_spec),
                         out_specs=(P(), P(), P()), check_vma=False)
```

```python
import functools

import jax
import jax.numpy as jnp
from jax import lax
from jax.experimental import pallas as pl
from jax.experimental.pallas import tpu as pltpu
from jax.sharding import PartitionSpec as P

BF = jnp.bfloat16
F32 = jnp.float32
BLK = 64
NEG = -1e30


def ring_order(n):
    return sorted(range(1, n), key=lambda d: (min(d, n - d), d))


def pack(v):
    out = []
    lane = lax.broadcasted_iota(jnp.int32, (BLK // 2, 128), 1)
    for k in range(v.shape[0] // BLK):
        lo, hi = v[k * BLK:(k + 1) * BLK, :128], v[k * BLK:(k + 1) * BLK, 128:]
        out += [lo, jnp.where(lane < 64, hi[:BLK // 2], pltpu.roll(hi[BLK // 2:], 64, 1))]
    return jnp.concatenate(out, axis=0)


def unpack(p):
    lane = lax.broadcasted_iota(jnp.int32, (BLK // 2, 128), 1)
    t = p[BLK:]
    hi = jnp.concatenate([jnp.where(lane < 64, t, 0.0), jnp.where(lane < 64, pltpu.roll(t, 64, 1), 0.0)], axis=0)
    return jnp.concatenate([p[:BLK], hi], axis=1)


def step_kernel(ZN, YN, XN, names, *refs):
    R = dict(zip(names, refs))
    a_hbm, x_ref, w1_ref, w2_ref = R["a"], R["x"], R["w1"], R["w2"]
    af, ab, at, w2p, mt = R["af"], R["ab"], R["at"], R["w2p"], R["mt"]
    rep_n, node_n = ZN * YN, 2 * XN
    r, i = lax.axis_index("rep"), lax.axis_index("nodes")
    z, y = r // YN, lax.rem(r, YN)
    x, c = i // 2, lax.rem(i, 2)
    classes, hidden = w2_ref.shape
    f_in = x_ref.shape[1]
    PB = 96

    def dev(dz=0, dy=0, dx=0, dc=0):
        return {"rep": lax.rem(z + dz, ZN) * YN + lax.rem(y + dy, YN),
                "nodes": lax.rem(x + dx, XN) * 2 + lax.rem(c + dc, 2)}

    def node_dev(e):
        return {"rep": r, "nodes": lax.rem(i + e, node_n)}

    def rows(k, n):
        return pl.ds(pl.multiple_of(k * n, n), n)

    z_order, y_order, x_order = ring_order(ZN), ring_order(YN), ring_order(XN)
    peers = [dev(dz=d) for d in z_order] + [dev(dy=d) for d in y_order] + [node_dev(e) for e in range(1, node_n)]

    rows_z = YN * BLK
    n_q = node_n * ZN

    @pl.loop(0, n_q)
    def _(q):
        pltpu.make_async_copy(
            a_hbm.at[rows(z, rows_z), pl.ds(pl.multiple_of(q * (YN * BLK) + (y // 2) * 128, 128), 128)],
            af.at[:, rows((lax.rem(q // ZN, 2) * ZN + lax.rem(q, ZN)) * XN + q // (2 * ZN), 128)], R["sem_af"]).start()

    barrier = pltpu.get_barrier_semaphore()
    for peer in peers:
        pl.semaphore_signal(barrier, inc=1, device_id=peer, device_id_type=pl.DeviceIdType.MESH)

    xg, yg, y2g, g2g, g1g = R["xg"], R["yg"], R["y2g"], R["g2g"], R["g1g"]
    own_f = (c * ZN + z) * XN + x
    xg[rows(own_f, BLK), :] = x_ref[...]
    mine_at = lax.rem(y, 2) * BLK

    @pl.loop(0, yg.shape[1] // 128)
    def _(k):
        zero_rows = pl.ds(pl.multiple_of(k * 128 + BLK - mine_at, BLK), BLK)
        for t in range(2):
            yg[t, zero_rows, :] = jnp.zeros((BLK, 256), BF)

    w2p[...] = jnp.zeros_like(w2p)
    w2p[:classes, :] = w2_ref[...].astype(BF)
    b1 = w1_ref[...].astype(BF)
    mask_row = R["msk"][...].astype(F32)
    mt[0] = jnp.broadcast_to(jnp.sum(mask_row, axis=1, keepdims=True), mt.shape[1:])

    pl.semaphore_wait(barrier, len(peers))

    pending = []

    def drain(keep):
        while len(pending) > keep:
            pending.pop(0).wait_send()

    def send(src, dst, ssem, rsem, device):
        cp = pltpu.make_async_remote_copy(src_ref=src, dst_ref=dst, send_sem=ssem, recv_sem=rsem,
                                          device_id=device, device_id_type=pl.DeviceIdType.MESH)
        cp.start()
        pending.append(cp)
        return cp

    def gather(g, buf, index, size, n, me, peer_of, done, hooks):
        zs, zr, ss, sr = R["zs"], R["zr"], R["ss"], R["sr"]

        def slot(zk):
            return buf.at[rows(index(zk, me), size)]

        def zof(k):
            return lax.rem(z + ZN - k, ZN)

        line = {}

        def spread(k):
            mine = slot(zof(k))
            line[k] = [send(mine, mine, ss.at[g, k, e], sr.at[g, k, e], peer_of(e)) for e in ring_order(n)]

        zc = {d: send(slot(z), slot(z), zs.at[g, d], zr.at[g, d], dev(dz=d)) for d in z_order[:2]}
        spread(0)
        zc.update({d: send(slot(z), slot(z), zs.at[g, d], zr.at[g, d], dev(dz=d)) for d in z_order[2:]})
        lines = [0] + z_order
        events = []
        for s, d in enumerate(z_order):
            events.append((True, d))
        events += [(False, k) for k in lines]
        for s, (first, k) in enumerate(events):
            hooks(s)
            if first:
                zc[k].wait_recv()
                spread(k)
            else:
                for cp in line[k]:
                    cp.wait_recv()
                done(zof(k), k)

    def start_ab():
        @pl.loop(0, node_n)
        def _(j):
            pltpu.make_async_copy(
                a_hbm.at[:, pl.ds(pl.multiple_of(j * (rep_n * BLK) + (r // 2) * 128, 128), 128)],
                ab.at[j], R["sem_ab"]).start()

    TR = min(512, at.shape[1])

    def transpose_part(j, q):
        if j == q == 0:
            pltpu.make_async_copy(ab, ab, R["sem_ab"]).wait()
        t = ab[(j % XN) * 2 + j // XN, q * TR:(q + 1) * TR, :].T

        @pl.when(lax.rem(r, 2) == 0)
        def _():
            at[j * BLK:(j + 1) * BLK, q * TR:(q + 1) * TR] = t[:BLK]

        @pl.when(lax.rem(r, 2) == 1)
        def _():
            at[j * BLK:(j + 1) * BLK, q * TR:(q + 1) * TR] = t[BLK:]

    fillers = [functools.partial(transpose_part, j, q) for j in range(node_n) for q in range(at.shape[1] // TR)]

    def fill(n):
        for _ in range(min(n, len(fillers))):
            fillers.pop(0)()

    def fill_hook(s):
        if s == 0:
            fill(4)

    def unpack_rows(buf, first_block, n, out, pitch=BLK, shift=0):
        for k in range(n):
            base = pl.multiple_of((first_block + k) * PB, 32)
            orow = pl.multiple_of((first_block + k) * pitch + shift, BLK)
            t = buf[pl.ds(base + BLK, BLK // 2), :]
            out[pl.ds(orow, BLK), :128] = buf[pl.ds(base, BLK), :]
            out[pl.ds(orow, BLK // 2), 128:] = t
            out[pl.ds(orow + BLK // 2, BLK // 2), 128:] = jnp.concatenate([t[:, 64:], t[:, :64]], axis=1)

    zacc = R["zacc"]

    def fwd_gather(g, buf, size, prepare, hooks):
        late = []

        def line(ck, zk):
            return buf.at[rows(ck * ZN + zk, XN * size)]

        def add(ck, zk, first):
            k = ck * ZN + zk
            if first and g == 0:
                pltpu.make_async_copy(af, af, R["sem_af"]).wait()
                start_ab()
            prepare(k)
            v = jnp.dot(af[:, rows(k, XN * 128)], yg[g, rows(k, XN * 128), :], preferred_element_type=F32)
            if first:
                zacc[...] = v
            else:
                zacc[...] += v

        def partner():
            cp, zk = late.pop(0)
            cp.wait_recv()
            add(1 - c, zk, False)

        def done(zk, k):
            mine = line(c, zk)
            late.append((send(mine, mine, R["cs"].at[g, k], R["cr"].at[g, k], dev(dc=1)), zk))
            add(c, zk, k == 0)
            if len(late) > 2:
                partner()

        gather(g, buf, lambda zk, xk: (c * ZN + zk) * XN + xk, size, XN, x, lambda e: dev(dx=e), done, hooks)
        while late:
            partner()

    def fwd_reduce(g, packed, n_fill):
        zp, zr = (R["zpp"], R["zrp"]) if packed else (R["zp"], R["zrw"])
        v = zacc[...]
        for k in range(YN):
            piece = v[k * BLK:(k + 1) * BLK]
            zp[k] = pack(piece) if packed else piece
        cps = [send(zp.at[lax.rem(y + e, YN)], zr.at[e], R["rs"].at[g, e], R["rr"].at[g, e], dev(dy=e)) for e in y_order]
        fill(n_fill)
        drain(len(cps))
        total = zp[y]
        for e, cp in zip(y_order, cps):
            cp.wait_recv()
            total = total + zr[e]
        return unpack(total) if packed else total

    def exchange_small(k, src, buf, order, peer_of):
        return [send(src, buf.at[e], R["ms"].at[k, e], R["mr"].at[k, e], peer_of(e)) for e in order]

    def small_sum(k, cps, order, buf, nxt):
        s = mt[k]
        for e, cp in zip(order, cps):
            cp.wait_recv()
            s = s + buf[e]
        mt[nxt] = s

    def y1_rows(k):
        rr = rows(k, XN * BLK)
        v = jnp.dot(xg[rr, :], b1, preferred_element_type=F32).astype(BF)
        for j in range(XN):
            yg[0, pl.ds(pl.multiple_of((k * XN + j) * 128 + mine_at, BLK), BLK), :] = v[j * BLK:(j + 1) * BLK]

    def y2_rows(k):
        unpack_rows(y2g, k * XN, XN, yg.at[1], 128, mine_at)

    mzc = []

    def count_hook(s):
        if s == 0:
            mzc.extend(exchange_small(0, mt.at[0], R["mz"], z_order, lambda e: dev(dz=e)))

    fwd_gather(0, xg, BLK, y1_rows, count_hook)
    small_sum(0, mzc, z_order, R["mz"], 1)
    mxc = exchange_small(1, mt.at[1], R["mx"], x_order, lambda e: dev(dx=e))
    z1 = fwd_reduce(0, False, 12)
    R["z1s"][...] = z1
    h1 = jnp.maximum(z1, 0.0).astype(BF)
    R["h1s"][...] = h1
    nt = (((1,), (1,)), ((), ()))
    y2 = lax.dot_general(h1, w2p[...], nt, preferred_element_type=F32)
    y2g[rows(own_f, PB), :] = pack(y2).astype(BF)
    small_sum(1, mxc, x_order, R["mx"], 2)
    myc = exchange_small(2, mt.at[2], R["my"], y_order, lambda e: dev(dy=e))
    fwd_gather(1, y2g, PB, y2_rows, fill_hook)
    small_sum(2, myc, y_order, R["my"], 3)
    mcc = exchange_small(3, mt.at[3], R["mc"], [1], lambda e: dev(dc=e))
    z2 = fwd_reduce(1, True, 11)
    small_sum(3, mcc, [1], R["mc"], 4)

    count = mt[4][:1, :1]
    diag = lax.broadcasted_iota(jnp.int32, (BLK, BLK), 0) == lax.broadcasted_iota(jnp.int32, (BLK, BLK), 1)
    labf = jnp.sum(jnp.where(diag, jnp.broadcast_to(R["lab"][...].astype(F32), (BLK, BLK)), 0.0), axis=1, keepdims=True)
    mskf = jnp.sum(jnp.where(diag, jnp.broadcast_to(mask_row, (BLK, BLK)), 0.0), axis=1, keepdims=True)
    lane = lax.broadcasted_iota(jnp.int32, z2.shape, 1)
    logits = jnp.where(lane < classes, z2, NEG)
    shifted = logits - jnp.max(logits, axis=1, keepdims=True)
    log_probs = shifted - jnp.log(jnp.sum(jnp.exp(shifted), axis=1, keepdims=True))
    onehot = jnp.where(lane.astype(F32) == labf, 1.0, 0.0)
    g2 = (jnp.exp(log_probs) - onehot) * (mskf / count)
    g2g[rows(r, PB), :] = pack(g2).astype(BF)
    local_loss = -jnp.sum(mskf * jnp.sum(onehot * log_probs, axis=1, keepdims=True), axis=0, keepdims=True)

    dacc = R["dacc"]

    def bwd(g, buf, size, packed, hooks, late=lambda: None):
        gu = R["gu"] if packed else buf

        def done(zk, k):
            if packed:
                unpack_rows(buf, zk * YN, YN, gu)
            rr = rows(zk, YN * BLK)
            v = jnp.dot(at[:, rr], gu[rr, :], preferred_element_type=F32)
            if k == 0:
                dacc[...] = v
            else:
                dacc[...] += v

        gather(g, buf, lambda zk, yk: zk * YN + yk, size, YN, y, lambda e: dev(dy=e), done, hooks)
        dp, dr, dsum, dx = (R["dpp"], R["drp"], R["dsp"], R["dxp"]) if packed else (R["dp"], R["dr"], R["ds"], R["dx"])
        for k in range(2):
            for j in range(XN):
                piece = dacc[(k * XN + j) * BLK:(k * XN + j + 1) * BLK]
                dp[k, j] = pack(piece) if packed else piece
        cp = send(dp.at[1 - c], dr, R["cs"].at[g, 0], R["cr"].at[g, 0], dev(dc=1))
        cp.wait_recv()
        dsum[...] = dp[c] + dr[...]
        cps = [send(dsum.at[lax.rem(x + e, XN)], dx.at[e], R["rs"].at[g, e], R["rr"].at[g, e], dev(dx=e)) for e in x_order]
        late()
        drain(len(cps) + 3)
        total = dsum[x]
        for e, cp in zip(x_order, cps):
            cp.wait_recv()
            total = total + dx[e]
        return (unpack(total) if packed else total).astype(BF)

    def all_reduce(t, pay, payx, payy, payz, fin, whole):
        rx = pay.shape[0] // node_n
        ry = rx // YN
        fs, fr = R["fs"], R["fr"]
        state = {}
        others = range(1, node_n)
        small = pl.ds(pl.multiple_of(i * rx + y * ry, 8), ry)

        def total(first, buf, order):
            for e, cp in zip(order, state["cp"]):
                cp.wait_recv()
                first = first + buf[e]
            return first

        def s0():
            state["cp"] = [send(pay.at[rows(lax.rem(i + e, node_n), rx)], payx.at[e], fs.at[t, 0, e], fr.at[t, 0, e], node_dev(e)) for e in others]

        def w1():
            payy[y] = total(pay[rows(i, rx)], payx, others)
            state["cp"] = [send(payy.at[y], payy.at[y], fs.at[t, 1, e], fr.at[t, 1, e], dev(dy=e)) for e in y_order]

        def in_order(buf, n):
            for cp in state["cp"]:
                cp.wait_recv()
            s = buf[0]
            for k in range(1, n):
                s = s + buf[k]
            return s

        def w2():
            payz[z] = in_order(payy, YN)
            state["cp"] = [send(payz.at[z], payz.at[z], fs.at[t, 2, d], fr.at[t, 2, d], dev(dz=d)) for d in z_order]

        def w3():
            fin[rows(i, rx)] = in_order(payz, ZN)
            mine = fin.at[rows(i, rx)]
            state["cp"] = [send(mine, mine, fs.at[t, 4, e], fr.at[t, 4, e], node_dev(e)) for e in others]

        def s1():
            payx[0] = total(pay[rows(i, rx)], payx, others)
            state["cp"] = [send(payx.at[0, rows(lax.rem(y + e, YN), ry)], payy.at[e], fs.at[t, 1, e], fr.at[t, 1, e], dev(dy=e)) for e in y_order]

        def s2():
            payz[z] = total(payx[0, rows(y, ry)], payy, y_order)
            state["cp"] = [send(payz.at[z], payz.at[z], fs.at[t, 2, d], fr.at[t, 2, d], dev(dz=d)) for d in z_order]

        def s3():
            for cp in state["cp"]:
                cp.wait_recv()
            s = payz[0]
            for k in range(1, ZN):
                s = s + payz[k]
            fin[small] = s
            state["cp"] = [send(fin.at[small], fin.at[small], fs.at[t, 3, e], fr.at[t, 3, e], dev(dy=e)) for e in y_order]

        def s4():
            for cp in state["cp"]:
                cp.wait_recv()
            mine = fin.at[rows(i, rx)]
            state["cp"] = [send(mine, mine, fs.at[t, 4, e], fr.at[t, 4, e], node_dev(e)) for e in others]

        def s5():
            for cp in state["cp"]:
                cp.wait_recv()

        return [s0, w1, w2, w3, s5] if whole else [s0, s1, s2, s3, s4, s5]

    d2 = bwd(2, g2g, PB, True, lambda s: fill(99) if s == 0 else None)
    tn = (((0,), (0,)), ((), ()))
    dh1 = jnp.dot(d2, w2p[...], preferred_element_type=F32)
    g1g[rows(r, BLK), :] = jnp.where(R["z1s"][...] > 0, dh1, 0.0).astype(BF)
    R["d2s"][...] = d2
    ar2 = all_reduce(0, R["pay2"], R["payx2"], R["payy2"], R["payz2"], R["fin2"], False)

    def make_dw2():
        dw2 = lax.dot_general(R["d2s"][...], R["h1s"][...], tn, preferred_element_type=F32)
        row = lax.broadcasted_iota(jnp.int32, (256, 128), 0)
        lane2 = lax.broadcasted_iota(jnp.int32, (256, 128), 1)
        R["pay2"][0:256] = jnp.where(jnp.logical_and(row == 255, lane2 == 127), local_loss, dw2[:, :128])
        R["pay2"][256:512] = dw2[:, 128:]
        ar2[0]()

    def beside_hook(s):
        if s == 0:
            make_dw2()

    d1 = bwd(3, g1g, BLK, False, beside_hook, ar2[1])
    dw1 = lax.dot_general(x_ref[...], d1, tn, preferred_element_type=F32)
    R["pay1"][0:f_in] = dw1[:, :128]
    R["pay1"][f_in:2 * f_in] = dw1[:, 128:]
    ar1 = all_reduce(1, R["pay1"], R["payx1"], R["payy1"], R["payz1"], R["fin1"], True)
    for s in range(5):
        ar1[s]()
        if s < 4:
            ar2[2 + s]()
    R["o1"][...] = R["fin1"][...]
    R["o2"][...] = R["fin2"][...]
    R["cnt"][...] = mt[4]
    for cp in pending:
        cp.wait_send()


def write_outputs(fin1, fin2, count, loss_ref, dw1_ref, dw2_ref):
    f_in, classes = dw1_ref.shape[0], dw2_ref.shape[0]
    dw2_ref[:, :128] = fin2[0:classes]
    dw2_ref[:, 128:] = fin2[256:256 + classes]
    loss_ref[0, 0] = jnp.sum(fin2[255:256, 127:] / count[:1, :1])
    dw1_ref[:, :128] = fin1[0:f_in]
    dw1_ref[:, 128:] = fin1[f_in:2 * f_in]


def solution(mesh):
    rep_n, node_n = mesh.shape["rep"], mesh.shape["nodes"]
    YN = 4
    ZN = rep_n // YN
    XN = node_n // 2

    def local_step(adj, features, w_one, w_two, labels, mask):
        f_in, hidden = w_one.shape
        classes = w_two.shape[1]
        rows_g = adj.shape[0]
        blocks_y = node_n * ZN
        V = pltpu.VMEM
        D = pltpu.SemaphoreType.DMA

        def reduce_bufs(t, n, cut):
            rx = n // node_n
            return {f"pay{t}": V((n, 128), F32), f"payx{t}": V((node_n, rx, 128), F32),
                    f"payy{t}": V((YN, rx // cut, 128), F32), f"payz{t}": V((ZN, rx // cut, 128), F32), f"fin{t}": V((n, 128), F32)}

        scratch = dict(
            af=V((YN * BLK, blocks_y * 128), BF),
            ab=V((node_n, rows_g, 128), BF), at=V((node_n * BLK, rows_g), BF),
            xg=V((blocks_y * BLK, f_in), BF), yg=V((2, blocks_y * 128, 256), BF), y2g=V((blocks_y * 96, 128), BF),
            g2g=V((rep_n * 96, 128), BF), gu=V((rows_g, 256), BF), g1g=V((rows_g, hidden), BF),
            zacc=V((YN * BLK, 256), F32), dacc=V((node_n * BLK, 256), F32),
            zp=V((YN, BLK, 256), F32), zrw=V((YN, BLK, 256), F32), zpp=V((YN, 96, 128), F32), zrp=V((YN, 96, 128), F32),
            dp=V((2, XN, BLK, 256), F32), dr=V((XN, BLK, 256), F32), ds=V((XN, BLK, 256), F32), dx=V((XN, BLK, 256), F32),
            dpp=V((2, XN, 96, 128), F32), drp=V((XN, 96, 128), F32), dsp=V((XN, 96, 128), F32), dxp=V((XN, 96, 128), F32),
            mt=V((5, 8, 128), F32), mz=V((ZN, 8, 128), F32), mx=V((XN, 8, 128), F32), my=V((YN, 8, 128), F32),
            mc=V((2, 8, 128), F32),
            z1s=V((BLK, hidden), F32), h1s=V((BLK, hidden), BF), d2s=V((BLK, 256), BF), w2p=V((256, hidden), BF),
            sem_af=D, sem_ab=D,
            zs=D((4, 8)), zr=D((4, 8)), ss=D((4, 8, 4)), sr=D((4, 8, 4)), cs=D((4, 8)), cr=D((4, 8)),
            rs=D((4, 4)), rr=D((4, 4)), ms=D((4, 8)), mr=D((4, 8)), fs=D((2, 7, 8)), fr=D((2, 7, 8)),
        )
        scratch.update(reduce_bufs(1, 2 * f_in, 1))
        scratch.update(reduce_bufs(2, 512, YN))
        names = ["a", "x", "w1", "w2", "lab", "msk", "o1", "o2", "cnt"] + list(scratch)
        vm = pl.BlockSpec(memory_space=pltpu.VMEM)
        sums = pl.pallas_call(
            functools.partial(step_kernel, ZN, YN, XN, names),
            out_shape=(jax.ShapeDtypeStruct((2 * f_in, 128), F32), jax.ShapeDtypeStruct((512, 128), F32),
                       jax.ShapeDtypeStruct((8, 128), F32)),
            in_specs=[pl.BlockSpec(memory_space=pl.ANY), vm, vm, vm, vm, vm],
            out_specs=(vm, vm, vm),
            scratch_shapes=list(scratch.values()),
            compiler_params=pltpu.CompilerParams(collective_id=0, has_side_effects=True, vmem_limit_bytes=60 * 2 ** 20),
            name="gcn_step",
        )(adj, features, w_one, w_two.T, labels.reshape(1, BLK), mask.reshape(1, BLK))
        loss, dw1, dw2 = pl.pallas_call(
            write_outputs,
            out_shape=(jax.ShapeDtypeStruct((1, 1), F32), jax.ShapeDtypeStruct((f_in, hidden), F32),
                       jax.ShapeDtypeStruct((classes, hidden), F32)),
            in_specs=[vm, vm, vm],
            out_specs=(pl.BlockSpec(memory_space=pltpu.SMEM), vm, vm),
            name="write_outputs",
        )(*sums)
        return loss.reshape(()), dw1, dw2.T

    row_spec = P(("nodes", "rep"))
    return jax.shard_map(local_step, mesh=mesh, in_specs=(P("nodes", None), P(("nodes", "rep"), None), P(), P(), row_spec, row_spec),
                         out_specs=(P(), P(), P()), check_vma=False)
```

```python
import functools

import jax
import jax.numpy as jnp
from jax import lax
from jax.experimental import pallas as pl
from jax.experimental.pallas import tpu as pltpu
from jax.sharding import PartitionSpec as P

BF = jnp.bfloat16
F32 = jnp.float32
BLK = 64
NEG = -1e30


def ring_order(n):
    if n == 4:
        return [2, 1, 3]
    return sorted(range(1, n), key=lambda d: (min(d, n - d), d))


def pack(v):
    out = []
    lane = lax.broadcasted_iota(jnp.int32, (BLK // 2, 128), 1)
    for k in range(v.shape[0] // BLK):
        lo, hi = v[k * BLK:(k + 1) * BLK, :128], v[k * BLK:(k + 1) * BLK, 128:]
        out += [lo, jnp.where(lane < 64, hi[:BLK // 2], pltpu.roll(hi[BLK // 2:], 64, 1))]
    return jnp.concatenate(out, axis=0)


def unpack(p):
    lane = lax.broadcasted_iota(jnp.int32, (BLK // 2, 128), 1)
    t = p[BLK:]
    hi = jnp.concatenate([jnp.where(lane < 64, t, 0.0), jnp.where(lane < 64, pltpu.roll(t, 64, 1), 0.0)], axis=0)
    return jnp.concatenate([p[:BLK], hi], axis=1)


def step_kernel(ZN, YN, XN, names, *refs):
    R = dict(zip(names, refs))
    a_hbm, x_ref, w1_ref, w2_ref = R["a"], R["x"], R["w1"], R["w2"]
    af, ab, at, w2p, mt = R["af"], R["ab"], R["at"], R["w2p"], R["mt"]
    rep_n, node_n = ZN * YN, 2 * XN
    r, i = lax.axis_index("rep"), lax.axis_index("nodes")
    z, y = r // YN, lax.rem(r, YN)
    x, c = i // 2, lax.rem(i, 2)
    classes, hidden = w2_ref.shape
    f_in = x_ref.shape[1]
    PB = 96

    def dev(dz=0, dy=0, dx=0, dc=0):
        return {"rep": lax.rem(z + dz, ZN) * YN + lax.rem(y + dy, YN),
                "nodes": lax.rem(x + dx, XN) * 2 + lax.rem(c + dc, 2)}

    def node_dev(e):
        return {"rep": r, "nodes": lax.rem(i + e, node_n)}

    def rows(k, n):
        return pl.ds(pl.multiple_of(k * n, n), n)

    z_order, y_order, x_order = ring_order(ZN), ring_order(YN), ring_order(XN)
    peers = [dev(dz=d) for d in z_order] + [dev(dy=d) for d in y_order] + [node_dev(e) for e in range(1, node_n)]

    rows_z = YN * BLK
    n_q = node_n * ZN

    @pl.loop(0, n_q)
    def _(q):
        pltpu.make_async_copy(
            a_hbm.at[rows(z, rows_z), pl.ds(pl.multiple_of(q * (YN * BLK) + (y // 2) * 128, 128), 128)],
            af.at[:, rows((lax.rem(q // ZN, 2) * ZN + lax.rem(q, ZN)) * XN + q // (2 * ZN), 128)], R["sem_af"]).start()

    barrier = pltpu.get_barrier_semaphore()
    for peer in peers:
        pl.semaphore_signal(barrier, inc=1, device_id=peer, device_id_type=pl.DeviceIdType.MESH)

    xg, yg, y2g, g2g, g1g = R["xg"], R["yg"], R["y2g"], R["g2g"], R["g1g"]
    own_f = (c * ZN + z) * XN + x
    xg[rows(own_f, BLK), :] = x_ref[...]
    mine_at = lax.rem(y, 2) * BLK

    @pl.loop(0, yg.shape[1] // 128)
    def _(k):
        zero_rows = pl.ds(pl.multiple_of(k * 128 + BLK - mine_at, BLK), BLK)
        for t in range(2):
            yg[t, zero_rows, :] = jnp.zeros((BLK, 256), BF)

    w2p[...] = jnp.zeros_like(w2p)
    w2p[:classes, :] = w2_ref[...].astype(BF)
    b1 = w1_ref[...].astype(BF)
    mask_row = R["msk"][...].astype(F32)
    mt[0] = jnp.broadcast_to(jnp.sum(mask_row, axis=1, keepdims=True), mt.shape[1:])

    pl.semaphore_wait(barrier, len(peers))

    pending = []

    def drain(keep):
        while len(pending) > keep:
            pending.pop(0).wait_send()

    def send(src, dst, ssem, rsem, device):
        cp = pltpu.make_async_remote_copy(src_ref=src, dst_ref=dst, send_sem=ssem, recv_sem=rsem,
                                          device_id=device, device_id_type=pl.DeviceIdType.MESH)
        cp.start()
        pending.append(cp)
        return cp

    def gather(g, buf, index, size, n, me, peer_of, done, hooks):
        zs, zr, ss, sr = R["zs"], R["zr"], R["ss"], R["sr"]

        def slot(zk):
            return buf.at[rows(index(zk, me), size)]

        def zof(k):
            return lax.rem(z + ZN - k, ZN)

        line = {}

        def spread(k):
            mine = slot(zof(k))
            line[k] = [send(mine, mine, ss.at[g, k, e], sr.at[g, k, e], peer_of(e)) for e in ring_order(n)]

        zc = {d: send(slot(z), slot(z), zs.at[g, d], zr.at[g, d], dev(dz=d)) for d in z_order[:2]}
        spread(0)
        zc.update({d: send(slot(z), slot(z), zs.at[g, d], zr.at[g, d], dev(dz=d)) for d in z_order[2:]})
        lines = [0] + z_order
        events = []
        for s, d in enumerate(z_order):
            events.append((True, d))
        events += [(False, k) for k in lines]
        for s, (first, k) in enumerate(events):
            hooks(s)
            if first:
                zc[k].wait_recv()
                spread(k)
            else:
                for cp in line[k]:
                    cp.wait_recv()
                done(zof(k), k)

    def start_ab():
        @pl.loop(0, node_n)
        def _(j):
            pltpu.make_async_copy(
                a_hbm.at[:, pl.ds(pl.multiple_of(j * (rep_n * BLK) + (r // 2) * 128, 128), 128)],
                ab.at[j], R["sem_ab"]).start()

    TR = min(512, at.shape[1])

    def transpose_part(j, q):
        if j == q == 0:
            pltpu.make_async_copy(ab, ab, R["sem_ab"]).wait()
        t = ab[(j % XN) * 2 + j // XN, q * TR:(q + 1) * TR, :].T

        @pl.when(lax.rem(r, 2) == 0)
        def _():
            at[j * BLK:(j + 1) * BLK, q * TR:(q + 1) * TR] = t[:BLK]

        @pl.when(lax.rem(r, 2) == 1)
        def _():
            at[j * BLK:(j + 1) * BLK, q * TR:(q + 1) * TR] = t[BLK:]

    fillers = [functools.partial(transpose_part, j, q) for j in range(node_n) for q in range(at.shape[1] // TR)]

    def fill(n):
        for _ in range(min(n, len(fillers))):
            fillers.pop(0)()

    def fill_hook(s):
        if s == 0:
            fill(4)

    def unpack_rows(buf, first_block, n, out, pitch=BLK, shift=0):
        for k in range(n):
            base = pl.multiple_of((first_block + k) * PB, 32)
            orow = pl.multiple_of((first_block + k) * pitch + shift, BLK)
            t = buf[pl.ds(base + BLK, BLK // 2), :]
            out[pl.ds(orow, BLK), :128] = buf[pl.ds(base, BLK), :]
            out[pl.ds(orow, BLK // 2), 128:] = t
            out[pl.ds(orow + BLK // 2, BLK // 2), 128:] = jnp.concatenate([t[:, 64:], t[:, :64]], axis=1)

    zacc = R["zacc"]

    def fwd_gather(g, buf, size, prepare, hooks):
        late = []

        def line(ck, zk):
            return buf.at[rows(ck * ZN + zk, XN * size)]

        def add(ck, zk, first):
            k = ck * ZN + zk
            if first and g == 0:
                pltpu.make_async_copy(af, af, R["sem_af"]).wait()
                start_ab()
            prepare(k)
            v = jnp.dot(af[:, rows(k, XN * 128)], yg[g, rows(k, XN * 128), :], preferred_element_type=F32)
            if first:
                zacc[...] = v
            else:
                zacc[...] += v

        def partner():
            cp, zk = late.pop(0)
            cp.wait_recv()
            add(1 - c, zk, False)

        def done(zk, k):
            mine = line(c, zk)
            late.append((send(mine, mine, R["cs"].at[g, k], R["cr"].at[g, k], dev(dc=1)), zk))
            add(c, zk, k == 0)
            if len(late) > 2:
                partner()

        gather(g, buf, lambda zk, xk: (c * ZN + zk) * XN + xk, size, XN, x, lambda e: dev(dx=e), done, hooks)
        while late:
            partner()

    def fwd_reduce(g, packed, n_fill):
        zp, zr = (R["zpp"], R["zrp"]) if packed else (R["zp"], R["zrw"])
        v = zacc[...]
        for k in range(YN):
            piece = v[k * BLK:(k + 1) * BLK]
            zp[k] = pack(piece) if packed else piece
        cps = [send(zp.at[lax.rem(y + e, YN)], zr.at[e], R["rs"].at[g, e], R["rr"].at[g, e], dev(dy=e)) for e in y_order]
        fill(n_fill)
        drain(len(cps))
        total = zp[y]
        for e, cp in zip(y_order, cps):
            cp.wait_recv()
            total = total + zr[e]
        return unpack(total) if packed else total

    def exchange_small(k, src, buf, order, peer_of):
        return [send(src, buf.at[e], R["ms"].at[k, e], R["mr"].at[k, e], peer_of(e)) for e in order]

    def small_sum(k, cps, order, buf, nxt):
        s = mt[k]
        for e, cp in zip(order, cps):
            cp.wait_recv()
            s = s + buf[e]
        mt[nxt] = s

    def y1_rows(k):
        rr = rows(k, XN * BLK)
        v = jnp.dot(xg[rr, :], b1, preferred_element_type=F32).astype(BF)
        for j in range(XN):
            yg[0, pl.ds(pl.multiple_of((k * XN + j) * 128 + mine_at, BLK), BLK), :] = v[j * BLK:(j + 1) * BLK]

    def y2_rows(k):
        unpack_rows(y2g, k * XN, XN, yg.at[1], 128, mine_at)

    mzc = []

    def count_hook(s):
        if s == 0:
            mzc.extend(exchange_small(0, mt.at[0], R["mz"], z_order, lambda e: dev(dz=e)))

    fwd_gather(0, xg, BLK, y1_rows, count_hook)
    small_sum(0, mzc, z_order, R["mz"], 1)
    mxc = exchange_small(1, mt.at[1], R["mx"], x_order, lambda e: dev(dx=e))
    z1 = fwd_reduce(0, False, 12)
    R["z1s"][...] = z1
    h1 = jnp.maximum(z1, 0.0).astype(BF)
    R["h1s"][...] = h1
    nt = (((1,), (1,)), ((), ()))
    y2 = lax.dot_general(h1, w2p[...], nt, preferred_element_type=F32)
    y2g[rows(own_f, PB), :] = pack(y2).astype(BF)
    small_sum(1, mxc, x_order, R["mx"], 2)
    myc = exchange_small(2, mt.at[2], R["my"], y_order, lambda e: dev(dy=e))
    fwd_gather(1, y2g, PB, y2_rows, fill_hook)
    small_sum(2, myc, y_order, R["my"], 3)
    mcc = exchange_small(3, mt.at[3], R["mc"], [1], lambda e: dev(dc=e))
    z2 = fwd_reduce(1, True, 11)
    small_sum(3, mcc, [1], R["mc"], 4)

    count = mt[4][:1, :1]
    diag = lax.broadcasted_iota(jnp.int32, (BLK, BLK), 0) == lax.broadcasted_iota(jnp.int32, (BLK, BLK), 1)
    labf = jnp.sum(jnp.where(diag, jnp.broadcast_to(R["lab"][...].astype(F32), (BLK, BLK)), 0.0), axis=1, keepdims=True)
    mskf = jnp.sum(jnp.where(diag, jnp.broadcast_to(mask_row, (BLK, BLK)), 0.0), axis=1, keepdims=True)
    lane = lax.broadcasted_iota(jnp.int32, z2.shape, 1)
    logits = jnp.where(lane < classes, z2, NEG)
    shifted = logits - jnp.max(logits, axis=1, keepdims=True)
    log_probs = shifted - jnp.log(jnp.sum(jnp.exp(shifted), axis=1, keepdims=True))
    onehot = jnp.where(lane.astype(F32) == labf, 1.0, 0.0)
    g2 = (jnp.exp(log_probs) - onehot) * (mskf / count)
    g2g[rows(r, PB), :] = pack(g2).astype(BF)
    local_loss = -jnp.sum(mskf * jnp.sum(onehot * log_probs, axis=1, keepdims=True), axis=0, keepdims=True)

    dacc = R["dacc"]

    def bwd(g, buf, size, packed, hooks, late=lambda: None):
        gu = R["gu"] if packed else buf

        def done(zk, k):
            if packed:
                unpack_rows(buf, zk * YN, YN, gu)
            rr = rows(zk, YN * BLK)
            v = jnp.dot(at[:, rr], gu[rr, :], preferred_element_type=F32)
            if k == 0:
                dacc[...] = v
            else:
                dacc[...] += v

        gather(g, buf, lambda zk, yk: zk * YN + yk, size, YN, y, lambda e: dev(dy=e), done, hooks)
        dp, dr, dsum, dx = (R["dpp"], R["drp"], R["dsp"], R["dxp"]) if packed else (R["dp"], R["dr"], R["ds"], R["dx"])
        for k in range(2):
            for j in range(XN):
                piece = dacc[(k * XN + j) * BLK:(k * XN + j + 1) * BLK]
                dp[k, j] = pack(piece) if packed else piece
        cp = send(dp.at[1 - c], dr, R["cs"].at[g, 0], R["cr"].at[g, 0], dev(dc=1))
        cp.wait_recv()
        dsum[...] = dp[c] + dr[...]
        cps = [send(dsum.at[lax.rem(x + e, XN)], dx.at[e], R["rs"].at[g, e], R["rr"].at[g, e], dev(dx=e)) for e in x_order]
        late()
        drain(len(cps) + 3)
        total = dsum[x]
        for e, cp in zip(x_order, cps):
            cp.wait_recv()
            total = total + dx[e]
        return (unpack(total) if packed else total).astype(BF)

    def all_reduce(t, pay, payx, payy, payz, fin, whole):
        rx = pay.shape[0] // node_n
        ry = rx // YN
        fs, fr = R["fs"], R["fr"]
        state = {}
        others = range(1, node_n)
        small = pl.ds(pl.multiple_of(i * rx + y * ry, 8), ry)

        def total(first, buf, order):
            for e, cp in zip(order, state["cp"]):
                cp.wait_recv()
                first = first + buf[e]
            return first

        def s0():
            state["cp"] = [send(pay.at[rows(lax.rem(i + e, node_n), rx)], payx.at[e], fs.at[t, 0, e], fr.at[t, 0, e], node_dev(e)) for e in others]

        def w1():
            payy[y] = total(pay[rows(i, rx)], payx, others)
            state["cp"] = [send(payy.at[y], payy.at[y], fs.at[t, 1, e], fr.at[t, 1, e], dev(dy=e)) for e in y_order]

        def in_order(buf, n):
            for cp in state["cp"]:
                cp.wait_recv()
            s = buf[0]
            for k in range(1, n):
                s = s + buf[k]
            return s

        def w2():
            payz[z] = in_order(payy, YN)
            state["cp"] = [send(payz.at[z], payz.at[z], fs.at[t, 2, d], fr.at[t, 2, d], dev(dz=d)) for d in z_order]

        def w3():
            fin[rows(i, rx)] = in_order(payz, ZN)
            mine = fin.at[rows(i, rx)]
            state["cp"] = [send(mine, mine, fs.at[t, 4, e], fr.at[t, 4, e], node_dev(e)) for e in others]

        def s1():
            payx[0] = total(pay[rows(i, rx)], payx, others)
            state["cp"] = [send(payx.at[0, rows(lax.rem(y + e, YN), ry)], payy.at[e], fs.at[t, 1, e], fr.at[t, 1, e], dev(dy=e)) for e in y_order]

        def s2():
            payz[z] = total(payx[0, rows(y, ry)], payy, y_order)
            state["cp"] = [send(payz.at[z], payz.at[z], fs.at[t, 2, d], fr.at[t, 2, d], dev(dz=d)) for d in z_order]

        def s3():
            for cp in state["cp"]:
                cp.wait_recv()
            s = payz[0]
            for k in range(1, ZN):
                s = s + payz[k]
            fin[small] = s
            state["cp"] = [send(fin.at[small], fin.at[small], fs.at[t, 3, e], fr.at[t, 3, e], dev(dy=e)) for e in y_order]

        def s4():
            for cp in state["cp"]:
                cp.wait_recv()
            mine = fin.at[rows(i, rx)]
            state["cp"] = [send(mine, mine, fs.at[t, 4, e], fr.at[t, 4, e], node_dev(e)) for e in others]

        def s5():
            for cp in state["cp"]:
                cp.wait_recv()

        return [s0, w1, w2, w3, s5] if whole else [s0, s1, s2, s3, s4, s5]

    d2 = bwd(2, g2g, PB, True, lambda s: fill(99) if s == 0 else None)
    tn = (((0,), (0,)), ((), ()))
    dh1 = jnp.dot(d2, w2p[...], preferred_element_type=F32)
    g1g[rows(r, BLK), :] = jnp.where(R["z1s"][...] > 0, dh1, 0.0).astype(BF)
    R["d2s"][...] = d2
    ar2 = all_reduce(0, R["pay2"], R["payx2"], R["payy2"], R["payz2"], R["fin2"], False)

    def make_dw2():
        dw2 = lax.dot_general(R["d2s"][...], R["h1s"][...], tn, preferred_element_type=F32)
        row = lax.broadcasted_iota(jnp.int32, (256, 128), 0)
        lane2 = lax.broadcasted_iota(jnp.int32, (256, 128), 1)
        R["pay2"][0:256] = jnp.where(jnp.logical_and(row == 255, lane2 == 127), local_loss, dw2[:, :128])
        R["pay2"][256:512] = dw2[:, 128:]
        ar2[0]()

    def beside_hook(s):
        if s == 0:
            make_dw2()

    d1 = bwd(3, g1g, BLK, False, beside_hook, ar2[1])
    dw1 = lax.dot_general(x_ref[...], d1, tn, preferred_element_type=F32)
    R["pay1"][0:f_in] = dw1[:, :128]
    R["pay1"][f_in:2 * f_in] = dw1[:, 128:]
    ar1 = all_reduce(1, R["pay1"], R["payx1"], R["payy1"], R["payz1"], R["fin1"], True)
    for s in range(5):
        ar1[s]()
        if s < 4:
            ar2[2 + s]()
    R["o1"][...] = R["fin1"][...]
    R["o2"][...] = R["fin2"][...]
    R["cnt"][...] = mt[4]
    for cp in pending:
        cp.wait_send()


def write_outputs(fin1, fin2, count, loss_ref, dw1_ref, dw2_ref):
    f_in, classes = dw1_ref.shape[0], dw2_ref.shape[0]
    dw2_ref[:, :128] = fin2[0:classes]
    dw2_ref[:, 128:] = fin2[256:256 + classes]
    loss_ref[0, 0] = jnp.sum(fin2[255:256, 127:] / count[:1, :1])
    dw1_ref[:, :128] = fin1[0:f_in]
    dw1_ref[:, 128:] = fin1[f_in:2 * f_in]


def solution(mesh):
    rep_n, node_n = mesh.shape["rep"], mesh.shape["nodes"]
    YN = 4
    ZN = rep_n // YN
    XN = node_n // 2

    def local_step(adj, features, w_one, w_two, labels, mask):
        f_in, hidden = w_one.shape
        classes = w_two.shape[1]
        rows_g = adj.shape[0]
        blocks_y = node_n * ZN
        V = pltpu.VMEM
        D = pltpu.SemaphoreType.DMA

        def reduce_bufs(t, n, cut):
            rx = n // node_n
            return {f"pay{t}": V((n, 128), F32), f"payx{t}": V((node_n, rx, 128), F32),
                    f"payy{t}": V((YN, rx // cut, 128), F32), f"payz{t}": V((ZN, rx // cut, 128), F32), f"fin{t}": V((n, 128), F32)}

        scratch = dict(
            af=V((YN * BLK, blocks_y * 128), BF),
            ab=V((node_n, rows_g, 128), BF), at=V((node_n * BLK, rows_g), BF),
            xg=V((blocks_y * BLK, f_in), BF), yg=V((2, blocks_y * 128, 256), BF), y2g=V((blocks_y * 96, 128), BF),
            g2g=V((rep_n * 96, 128), BF), gu=V((rows_g, 256), BF), g1g=V((rows_g, hidden), BF),
            zacc=V((YN * BLK, 256), F32), dacc=V((node_n * BLK, 256), F32),
            zp=V((YN, BLK, 256), F32), zrw=V((YN, BLK, 256), F32), zpp=V((YN, 96, 128), F32), zrp=V((YN, 96, 128), F32),
            dp=V((2, XN, BLK, 256), F32), dr=V((XN, BLK, 256), F32), ds=V((XN, BLK, 256), F32), dx=V((XN, BLK, 256), F32),
            dpp=V((2, XN, 96, 128), F32), drp=V((XN, 96, 128), F32), dsp=V((XN, 96, 128), F32), dxp=V((XN, 96, 128), F32),
            mt=V((5, 8, 128), F32), mz=V((ZN, 8, 128), F32), mx=V((XN, 8, 128), F32), my=V((YN, 8, 128), F32),
            mc=V((2, 8, 128), F32),
            z1s=V((BLK, hidden), F32), h1s=V((BLK, hidden), BF), d2s=V((BLK, 256), BF), w2p=V((256, hidden), BF),
            sem_af=D, sem_ab=D,
            zs=D((4, 8)), zr=D((4, 8)), ss=D((4, 8, 4)), sr=D((4, 8, 4)), cs=D((4, 8)), cr=D((4, 8)),
            rs=D((4, 4)), rr=D((4, 4)), ms=D((4, 8)), mr=D((4, 8)), fs=D((2, 7, 8)), fr=D((2, 7, 8)),
        )
        scratch.update(reduce_bufs(1, 2 * f_in, 1))
        scratch.update(reduce_bufs(2, 512, YN))
        names = ["a", "x", "w1", "w2", "lab", "msk", "o1", "o2", "cnt"] + list(scratch)
        vm = pl.BlockSpec(memory_space=pltpu.VMEM)
        sums = pl.pallas_call(
            functools.partial(step_kernel, ZN, YN, XN, names),
            out_shape=(jax.ShapeDtypeStruct((2 * f_in, 128), F32), jax.ShapeDtypeStruct((512, 128), F32),
                       jax.ShapeDtypeStruct((8, 128), F32)),
            in_specs=[pl.BlockSpec(memory_space=pl.ANY), vm, vm, vm, vm, vm],
            out_specs=(vm, vm, vm),
            scratch_shapes=list(scratch.values()),
            compiler_params=pltpu.CompilerParams(collective_id=0, has_side_effects=True, vmem_limit_bytes=60 * 2 ** 20),
            name="gcn_step",
        )(adj, features, w_one, w_two.T, labels.reshape(1, BLK), mask.reshape(1, BLK))
        loss, dw1, dw2 = pl.pallas_call(
            write_outputs,
            out_shape=(jax.ShapeDtypeStruct((1, 1), F32), jax.ShapeDtypeStruct((f_in, hidden), F32),
                       jax.ShapeDtypeStruct((classes, hidden), F32)),
            in_specs=[vm, vm, vm],
            out_specs=(pl.BlockSpec(memory_space=pltpu.SMEM), vm, vm),
            name="write_outputs",
        )(*sums)
        return loss.reshape(()), dw1, dw2.T

    row_spec = P(("nodes", "rep"))
    return jax.shard_map(local_step, mesh=mesh, in_specs=(P("nodes", None), P(("nodes", "rep"), None), P(), P(), row_spec, row_spec),
                         out_specs=(P(), P(), P()), check_vma=False)
```
